256 devices in a mesh: samples: 32 (over y, z), variants: 8 (over x, core).
Axes of the slice: x: 4, y: 4, z: 8, core: 2. Of those that a mesh axis runs over, the one named last changes fastest.
Arguments:
- genotypes: int32 [4096, 131072], P('variants', 'samples'), may hold values from 0 to 3, as said below
- weights: float32 [131072], P('samples'), may hold values from 0.25 to 20
Outputs:
- call_mean: float32 [4096], P('variants')
- call_var: float32 [4096], P('variants')
- class_counts: int32 [4, 4096], P(None, 'variants')
- ld_window: float32 [1024, 4096], P('samples', 'variants')
- sample_calls: int32 [2, 131072], P(None, 'samples')
- sample_share: float32 [131072], P('samples')
The draws below stay inside these ranges and needn't reach their ends.
Inputs may be any that keep to these rules, and one draw needn't show every extreme that they name: `genotypes`: in every variant's row, each aligned group of 8 samples (samples 8 i to 8 i + 7) holds at least one call other than 3.
All inputs are finite; a program needn't handle non-finite values.
Results may differ from the reference program's by a relative error of at most 0.0004.
Values may be sent and summed in bfloat16 or wider, within the bound.
A program may use at most 64 MiB of HBM per device.

```python
import jax
import jax.numpy as jnp
from jax import lax

VAR_DEV = 512
VARIANTS = 4096
SAMPLES = 131072


def draw_genotypes(key, part):
    keys = jax.random.split(key, 6)
    level_all = jax.random.randint(keys[0], (VARIANTS,), 150, 500)
    hold_all = jax.random.randint(keys[1], (VARIANTS,), 300, 850)
    gap_all = jax.random.randint(keys[2], (VARIANTS,), 20, 400)
    step_keys = jax.random.split(keys[3], VARIANTS)
    slot = jnp.arange(SAMPLES, dtype=jnp.int32) % 8
    first_start = jax.random.randint(keys[4], (SAMPLES,), 0, 1000) < 300
    second_start = jax.random.randint(keys[5], (SAMPLES,), 0, 1000) < 300

    def advance(carry, inputs):
        first_hap, second_hap = carry
        step_key, level, hold, gap = inputs
        pieces = jax.random.split(step_key, 6)
        fresh_one = jax.random.randint(pieces[0], (SAMPLES,), 0, 1000) < level
        fresh_two = jax.random.randint(pieces[1], (SAMPLES,), 0, 1000) < level
        keep_one = jax.random.randint(pieces[2], (SAMPLES,), 0, 1000) < hold
        keep_two = jax.random.randint(pieces[3], (SAMPLES,), 0, 1000) < hold
        new_one = jnp.where(keep_one, first_hap, fresh_one)
        new_two = jnp.where(keep_two, second_hap, fresh_two)
        chosen = jnp.repeat(jax.random.randint(pieces[5], (SAMPLES // 8,), 0, 8), 8)
        lost = (jax.random.randint(pieces[4], (SAMPLES,), 0, 1000) < gap) & (slot != chosen)
        calls = jnp.where(lost, 3, new_one.astype(jnp.int32) + new_two.astype(jnp.int32))
        return ((new_one, new_two), calls.astype(jnp.int32))
    final_state, rows = lax.scan(advance, (first_start, second_start), (step_keys, level_all, hold_all, gap_all))
    return rows


def draw_weights(key, part):
    position = jnp.arange(SAMPLES, dtype=jnp.float32) / max(SAMPLES - 1, 1)
    base = jnp.exp(jax.random.uniform(key, (SAMPLES,), jnp.float32, jnp.log(0.3), jnp.log(3.0)))
    rise = 1.0 + 2.0 * position
    return (base * rise).astype(jnp.float32)


def setup_inputs(seed: int = 0) -> dict:
    key_list = jax.random.split(jax.random.key(seed), 3)
    genotypes = draw_genotypes(jax.random.fold_in(key_list[2], 71), 0)
    weights = draw_weights(jax.random.fold_in(key_list[2], 71), 0)
    return dict(genotypes=genotypes, weights=weights)


def reference(genotypes, weights):
    block_count = VARIANTS // VAR_DEV
    blocks = genotypes.reshape(block_count, VAR_DEV, SAMPLES)
    root_weight = jnp.sqrt(weights)

    def block_stats(block):
        present = block != 3
        called = present.astype(jnp.float32)
        dosage = jnp.where(present, block, 0).astype(jnp.float32)
        weighted = called * weights[None, :]
        w_sum = lax.optimization_barrier(jnp.sum(weighted, axis=1))
        mean_value = lax.optimization_barrier(jnp.sum(weighted * dosage, axis=1)) / w_sum
        centered = (dosage - mean_value[:, None]) * called
        var_value = lax.optimization_barrier(jnp.sum(weighted * centered * centered, axis=1)) / w_sum
        counts = jnp.stack([lax.optimization_barrier(jnp.sum((block == level).astype(jnp.int32), axis=1)) for level in range(4)])
        factor = 1.0 / jnp.sqrt(w_sum * (var_value + 1e-05))
        scaled = (root_weight[None, :] * centered * factor[:, None]).astype(jnp.bfloat16)
        return (mean_value, var_value, counts, scaled)
    mean_value, var_value, counts, scaled = lax.map(block_stats, blocks)
    padded = jnp.concatenate([scaled, jnp.zeros((1, VAR_DEV, SAMPLES), scaled.dtype)], axis=0)

    def window(index):
        own = lax.dynamic_index_in_dim(padded, index, 0, keepdims=False)
        after = lax.dynamic_index_in_dim(padded, index + 1, 0, keepdims=False)
        joined = jnp.concatenate([own, after], axis=0).astype(jnp.float32)
        return jnp.dot(joined, own.astype(jnp.float32).T, preferred_element_type=jnp.float32)
    ld_blocks = lax.map(window, jnp.arange(block_count, dtype=jnp.int32))
    ld_window = ld_blocks.transpose(1, 0, 2).reshape(2 * VAR_DEV, VARIANTS)

    def sample_block(block_pair):
        block, scaled_block = block_pair
        squares = scaled_block.astype(jnp.float32)
        return (lax.optimization_barrier(jnp.sum((block != 3).astype(jnp.int32), axis=0)), lax.optimization_barrier(jnp.sum((block == 1).astype(jnp.int32), axis=0)), lax.optimization_barrier(jnp.sum(squares * squares, axis=0)))
    called_rows, het_rows, square_rows = lax.map(sample_block, (blocks, scaled))
    sample_calls = jnp.stack([lax.optimization_barrier(jnp.sum(called_rows, axis=0)), lax.optimization_barrier(jnp.sum(het_rows, axis=0))])
    sample_share = lax.optimization_barrier(jnp.sum(square_rows, axis=0)) * (SAMPLES / VARIANTS)
    return (mean_value.reshape(VARIANTS), var_value.reshape(VARIANTS), counts.transpose(1, 0, 2).reshape(4, VARIANTS), ld_window, sample_calls, sample_share)
```

```python
import functools

import jax
import jax.numpy as jnp
from jax import lax
from jax.experimental import pallas as pl
from jax.experimental.pallas import tpu as pltpu
from jax.sharding import PartitionSpec as P

MESH = pl.DeviceIdType.MESH
LANES = 128
PARTS = 8
QUARTERS = 4
TILE = 16
HALF = jnp.float32
GAIN = 1.0
F32 = jnp.float32
NT = (((1,), (1,)), ((), ()))


def drain(ref, sem):
    pltpu.make_async_copy(ref, ref, sem).wait()


def folded(value):
    return sum(value[:, i : i + LANES] for i in range(0, value.shape[1], LANES))


def spread(value, width):
    return jnp.concatenate([value] * (width // LANES), axis=1)


def kernel(
    ny, nz, nv, samples_all,
    g_hbm, w_ref,
    mean_o, var_o, count_o, ld_o, calls_o, share_o,
    gbuf, raw, scl, recv_n, recv_p, wide_w, root_w, moments, codes, col, squares,
    crit_z, crit_y, cnt_z, cnt_y, mf, bcast, samp_s, samp_r, samp_g, acc,
    ysend, yrecv, zsend, zrecv, fin, fin_o, fin_n, fin_p,
    gsem, xs_n, xs_p, xr_n, xr_p, stat_s, stat_r, mf_s, mf_r, samp_ss, samp_rs,
    ys_sem, yr_sem, zs_sem, zr_sem, fo_s, fo_r, fn_s, fn_r, fp_s, fp_r,
):
    k, b = lax.axis_index("samples"), lax.axis_index("variants")
    y, z = k // nz, k % nz
    blocks = 4 * nz
    rows = blocks * TILE
    width = gbuf.shape[2] // PARTS
    half = PARTS // 2
    slice_w = gbuf.shape[2] // nv
    first, last = b == 0, b == nv - 1

    def at(ky, kz):
        return {"samples": ky * nz + kz}

    for part in range(8):
        group = pl.ds(part * (blocks // 8), blocks // 8)
        pltpu.make_async_copy(g_hbm.at[group], gbuf.at[group], gsem.at[part]).start()

    barrier = pltpu.get_barrier_semaphore()

    def greet(device):
        pl.semaphore_signal(barrier, inc=1, device_id=device, device_id_type=MESH)

    for d in range(1, ny):
        greet(at((y + d) % ny, z))
    for d in range(1, nz):
        greet(at(y, (z + d) % nz))
    for d in range(1, nv):
        greet({"variants": (b + d) % nv})

    @pl.when(b > 0)
    def _():
        for d in range(1, ny):
            greet({"samples": ((y + d) % ny) * nz + z, "variants": b - 1})

    @pl.when(b < nv - 1)
    def _():
        for d in range(1, ny):
            greet({"samples": ((y + d) % ny) * nz + z, "variants": b + 1})

    wide_w[...] = jnp.broadcast_to(w_ref[...], wide_w.shape)
    root_w[...] = jnp.sqrt(wide_w[...])
    col[...] = jnp.zeros_like(col)
    squares[...] = jnp.zeros_like(squares)

    def place(rb):
        return rb // (2 * nz), (rb // 2) % nz, rb % 2

    def first_pass(rb, carry):
        yr, zz, hh = place(rb)
        sum_w = jnp.zeros((TILE, LANES), F32)
        sum_1 = jnp.zeros((TILE, LANES), F32)
        sum_2 = jnp.zeros((TILE, LANES), F32)
        sum_c = jnp.zeros((TILE, LANES), jnp.int32)
        for kc in range(PARTS):
            cols = slice(kc * width, (kc + 1) * width)
            g = gbuf[rb, :, cols]
            gf = g.astype(F32)
            raw[kc, yr, zz, hh] = gf.astype(jnp.bfloat16)
            kept = jnp.where(g == 3, 0.0, wide_w[:, cols])
            once = kept * gf
            twice = once * gf
            code = jnp.left_shift(jnp.ones_like(g), g * 8)
            col[:, cols] += code[:8] + code[8:]
            sum_w += folded(kept)
            sum_1 += folded(once)
            sum_2 += folded(twice)
            sum_c += folded(code)
        moments[0, rb] = sum_w
        moments[1, rb] = sum_1
        moments[2, rb] = sum_2
        codes[rb] = sum_c
        return carry

    def copy_n(c):
        return pltpu.make_async_remote_copy(
            src_ref=raw.at[pl.ds(0, half), c // 2, :, c % 2],
            dst_ref=recv_n.at[c],
            send_sem=xs_n.at[c],
            recv_sem=xr_n.at[c],
            device_id={"variants": jnp.maximum(b - 1, 0)},
            device_id_type=MESH,
        )

    def copy_p(c):
        return pltpu.make_async_remote_copy(
            src_ref=raw.at[pl.ds(half, half), c // 2, pl.ds((c % 2) * (nz // 2), nz // 2)],
            dst_ref=recv_p.at[c],
            send_sem=xs_p.at[c],
            recv_sem=xr_p.at[c],
            device_id={"variants": jnp.minimum(b + 1, nv - 1)},
            device_id_type=MESH,
        )

    def wait_part(part):
        group = pl.ds(part * (blocks // 8), blocks // 8)
        pltpu.make_async_copy(g_hbm.at[group], gbuf.at[group], gsem.at[part]).wait()

    neighbours = jnp.where(b > 0, ny - 1, 0) + jnp.where(b < nv - 1, ny - 1, 0)
    for quarter in range(QUARTERS):
        for part in (2 * quarter, 2 * quarter + 1):
            wait_part(part)
            lax.fori_loop(part * (blocks // 8), (part + 1) * (blocks // 8), first_pass, 0)
        if quarter == 0:
            pl.semaphore_wait(barrier, (ny - 1) + (nz - 1) + (nv - 1) + neighbours)

        @pl.when(b < nv - 1)
        def _():
            copy_p(quarter).start()

        if quarter % 2 == 1:

            @pl.when(b > 0)
            def _():
                copy_n(quarter - 1).start()
                copy_n(quarter).start()

    def to_row(value):
        return jnp.sum(value.reshape(rows, LANES).T, axis=0, keepdims=True)

    def push(src, dst, i, device):
        return pltpu.make_async_remote_copy(
            src_ref=src,
            dst_ref=dst,
            send_sem=stat_s.at[i],
            recv_sem=stat_r.at[i],
            device_id=device,
            device_id_type=MESH,
        )

    for q in range(3):
        crit_z[z, q : q + 1, :] = to_row(moments[q])
    crit_z[z, 3:4, :] = jnp.zeros((1, rows), F32)
    for d in range(1, nz):
        push(crit_z.at[z], crit_z.at[z], 0, at(y, (z + d) % nz)).start()
    fields = codes[...]
    for level in range(4):
        field = jnp.bitwise_and(jnp.right_shift(fields, 8 * level), 255)
        cnt_z[z, level : level + 1, :] = to_row(field.astype(F32))
    for d in range(1, nz):
        push(cnt_z.at[z], cnt_z.at[z], 1, at(y, (z + d) % nz)).start()

    drain(crit_z.at[pl.ds(0, nz - 1)], stat_r.at[0])
    crit_y[y] = sum(crit_z[i] for i in range(nz))
    for d in range(1, ny):
        push(crit_y.at[y], crit_y.at[y], 2, at((y + d) % ny, z)).start()
    drain(cnt_z.at[pl.ds(0, nz - 1)], stat_r.at[1])
    cnt_y[y] = sum(cnt_z[i] for i in range(nz))
    for d in range(1, ny):
        push(cnt_y.at[y], cnt_y.at[y], 3, at((y + d) % ny, z)).start()
    drain(crit_y.at[pl.ds(0, ny - 1)], stat_r.at[2])
    total = sum(crit_y[i] for i in range(ny))
    w_sum, first_total, second_total = total[0:1], total[1:2], total[2:3]
    mean = first_total / w_sum
    var = (second_total - first_total * mean) / w_sum
    factor = 1.0 / jnp.sqrt(w_sum * (var + 1e-05))
    mean_o[...] = mean
    var_o[...] = var
    mf[0, 0:1, :] = mean
    mf[0, 1:2, :] = factor

    def mf_copy(slot, target):
        return pltpu.make_async_remote_copy(
            src_ref=mf.at[0],
            dst_ref=mf.at[slot],
            send_sem=mf_s.at[slot - 1],
            recv_sem=mf_r.at[slot - 1],
            device_id={"variants": target},
            device_id_type=MESH,
        )

    to_prev = mf_copy(1, jnp.maximum(b - 1, 0))
    to_next = mf_copy(2, jnp.minimum(b + 1, nv - 1))

    @pl.when(b > 0)
    def _():
        to_prev.start()

    @pl.when(b < nv - 1)
    def _():
        to_next.start()

    def widen(slot):
        for q in range(2):
            tall = jnp.broadcast_to(mf[slot, q : q + 1, :], (LANES, rows)).T
            bcast[slot, q] = tall.reshape(2, nz, 2, TILE, LANES)

    def scaled(value, roots, mean_rows, factor_rows):
        x = value.astype(F32)
        out = (roots * (x - spread(mean_rows, width))) * spread(factor_rows, width)
        return jnp.where(x > 2.5, 0.0, out).astype(jnp.bfloat16)

    widen(0)

    def second_pass(rb, carry):
        yr, zz, hh = place(rb)
        mean_rows, factor_rows = bcast[0, 0, yr, zz, hh], bcast[0, 1, yr, zz, hh]
        for kc in range(PARTS):
            cols = slice(kc * width, (kc + 1) * width)
            out = scaled(raw[kc, yr, zz, hh], root_w[:, cols], mean_rows, factor_rows)
            scl[kc, rb] = out
            wide = out.astype(F32)
            wide = wide * wide
            squares[:, cols] += wide[:8] + wide[8:]
        return carry

    lax.fori_loop(0, blocks, second_pass, 0)

    packed = col[...]
    missing = jnp.sum(jnp.bitwise_and(jnp.right_shift(packed, 24), 255), axis=0, keepdims=True)
    het = jnp.sum(jnp.bitwise_and(jnp.right_shift(packed, 8), 255), axis=0, keepdims=True)
    called = (rows - missing).astype(F32)
    het = het.astype(F32)
    share = jnp.sum(squares[...], axis=0, keepdims=True)
    for p in range(nv):
        cols = slice(p * slice_w, (p + 1) * slice_w)
        samp_s[p, 0:1, :] = called[:, cols]
        samp_s[p, 1:2, :] = het[:, cols]
        samp_s[p, 2:3, :] = share[:, cols]
        samp_s[p, 3:4, :] = jnp.zeros((1, slice_w), F32)
    samp_r[b] = samp_s[b]

    def samp_copy(i, src, dst, target):
        return pltpu.make_async_remote_copy(
            src_ref=src,
            dst_ref=dst,
            send_sem=samp_ss.at[i],
            recv_sem=samp_rs.at[i],
            device_id={"variants": target},
            device_id_type=MESH,
        )

    for d in range(1, nv):
        target = (b + d) % nv
        samp_copy(0, samp_s.at[target], samp_r.at[b], target).start()

    def y_copy(u, d):
        target = (y + d) % ny
        return pltpu.make_async_remote_copy(
            src_ref=ysend.at[u, target],
            dst_ref=yrecv.at[u, d - 1],
            send_sem=ys_sem.at[u],
            recv_sem=yr_sem.at[u],
            device_id=at(target, z),
            device_id_type=MESH,
        )

    def z_copy(u, d):
        target = (z + d) % nz
        return pltpu.make_async_remote_copy(
            src_ref=zsend.at[u, target],
            dst_ref=zrecv.at[u, d - 1],
            send_sem=zs_sem.at[u],
            recv_sem=zr_sem.at[u],
            device_id=at(y, target),
            device_id_type=MESH,
        )

    def y_start(u):
        for d in range(1, ny):
            y_copy(u, d).start()

    def y_fold(u):
        drain(yrecv.at[u], yr_sem.at[u])
        part = ysend[u, y].astype(F32)
        for d in range(ny - 1):
            part = part + yrecv[u, d].astype(F32)
        zsend[u] = part.astype(HALF)
        for d in range(1, nz):
            z_copy(u, d).start()

    def z_fold(u):
        drain(zrecv.at[u], zr_sem.at[u])
        part = zsend[u, z].astype(F32)
        for d in range(nz - 1):
            part = part + zrecv[u, d].astype(F32)
        fin[u] = part * (1.0 / GAIN)

    qw = rows // QUARTERS

    def group_rows(value, u):
        value = (value * GAIN).astype(HALF).reshape(2, nz, 2, TILE, qw)
        for yr in range(2):
            for hh in range(2):
                ysend[u, 2 * yr + hh] = value[yr, :, hh]

    for pair in range(2):
        acc[...] = jnp.zeros_like(acc)

        def own(kc, carry):
            left = scl[kc].reshape(rows, width)
            right = scl[kc, pair * (blocks // 2) : (pair + 1) * (blocks // 2)]
            acc[...] += lax.dot_general(
                left, right.reshape(rows // 2, width), NT, preferred_element_type=F32
            )
            return carry

        lax.fori_loop(0, PARTS, own, 0)
        for j in range(2):
            group_rows(acc[:, j * qw : (j + 1) * qw], 2 * pair + j)
            y_start(2 * pair + j)

    @pl.when(b < nv - 1)
    def _():
        to_prev.wait_recv()
        widen(1)

    @pl.when(b > 0)
    def _():
        to_next.wait_recv()
        widen(2)

    def chunk_n(c):
        copy_n(c).wait_recv()
        for kc in range(half):
            roots = root_w[:, kc * width : (kc + 1) * width]
            for zz in range(nz):
                recv_n[c, kc, zz] = scaled(
                    recv_n[c, kc, zz],
                    roots,
                    bcast[1, 0, c // 2, zz, c % 2],
                    bcast[1, 1, c // 2, zz, c % 2],
                )
        out = jnp.zeros((nz * TILE, rows), F32)
        for kc in range(half):
            out = out + lax.dot_general(
                recv_n[c, kc].reshape(nz * TILE, width),
                scl[kc].reshape(rows, width),
                NT,
                preferred_element_type=F32,
            )
        out = (out * GAIN).astype(HALF)
        for q in range(QUARTERS):
            ysend[4 + c, q] = out[:, q * qw : (q + 1) * qw].reshape(nz, TILE, qw)
        y_start(4 + c)

    def chunk_p(c):
        copy_p(c).wait_recv()
        for kc in range(half):
            roots = root_w[:, (half + kc) * width : (half + kc + 1) * width]
            for zz in range(nz // 2):
                for hh in range(2):
                    spot = (c // 2, (c % 2) * (nz // 2) + zz, hh)
                    recv_p[c, kc, zz, hh] = scaled(
                        recv_p[c, kc, zz, hh], roots, bcast[(2, 0, *spot)], bcast[(2, 1, *spot)]
                    )
        out = jnp.zeros((rows, qw), F32)
        for kc in range(half):
            out = out + lax.dot_general(
                scl[half + kc].reshape(rows, width),
                recv_p[c, kc].reshape(qw, width),
                NT,
                preferred_element_type=F32,
            )
        group_rows(out, 8 + c)
        y_start(8 + c)

    def n_copy(c):
        return pltpu.make_async_remote_copy(
            src_ref=fin.at[4 + c],
            dst_ref=fin_n.at[c % 2, y],
            send_sem=fn_s.at[c],
            recv_sem=fn_r.at[c % 2],
            device_id=at(2 + c // 2, z),
            device_id_type=MESH,
        )

    def o_copy():
        return pltpu.make_async_remote_copy(
            src_ref=fin.at[pl.ds(0, QUARTERS)],
            dst_ref=fin_o.at[y % 2],
            send_sem=fo_s.at[0],
            recv_sem=fo_r.at[y % 2],
            device_id=at(y // 2, z),
            device_id_type=MESH,
        )

    def p_copy():
        return pltpu.make_async_remote_copy(
            src_ref=fin.at[pl.ds(8, QUARTERS)],
            dst_ref=fin_p.at[y % 2],
            send_sem=fp_s.at[0],
            recv_sem=fp_r.at[y % 2],
            device_id={"samples": (2 + y // 2) * nz + z, "variants": jnp.maximum(b - 1, 0)},
            device_id_type=MESH,
        )

    def n_final(c):
        owner = 2 + c // 2

        @pl.when(y == owner)
        def _():
            fin_n[c % 2, y] = fin[4 + c]

        @pl.when(y != owner)
        def _():
            n_copy(c).start()

    def step(c, carry):
        @pl.when(c < QUARTERS)
        def _():
            @pl.when(b < nv - 1)
            def _():
                chunk_n(c)

            @pl.when(b > 0)
            def _():
                chunk_p(c)

        @pl.when(c == 0)
        def _():
            for u in range(QUARTERS):
                y_fold(u)

        @pl.when((c >= 1) & (c <= QUARTERS))
        def _():
            @pl.when(b < nv - 1)
            def _():
                y_fold(4 + c - 1)

            @pl.when(b > 0)
            def _():
                y_fold(8 + c - 1)

        @pl.when(c == 1)
        def _():
            for u in range(QUARTERS):
                z_fold(u)

            @pl.when(y == 0)
            def _():
                fin_o[0] = fin[0:QUARTERS]

            @pl.when(y > 0)
            def _():
                o_copy().start()

            drain(samp_r.at[pl.ds(0, nv - 1)], samp_rs.at[0])
            samp_g[b] = sum(samp_r[p] for p in range(nv))
            for d in range(1, nv):
                samp_copy(1, samp_g.at[b], samp_g.at[b], (b + d) % nv).start()

        @pl.when(c >= 2)
        def _():
            @pl.when(b < nv - 1)
            def _():
                z_fold(4 + c - 2)
                n_final(c - 2)

            @pl.when(b > 0)
            def _():
                z_fold(8 + c - 2)

        return carry

    lax.fori_loop(0, QUARTERS + 2, step, 0)

    @pl.when(b > 0)
    def _():
        p_copy().start()

    drain(cnt_y.at[pl.ds(0, ny - 1)], stat_r.at[3])
    count_o[...] = sum(cnt_y[i] for i in range(ny)).astype(jnp.int32)
    drain(samp_g.at[pl.ds(0, nv - 1)], samp_rs.at[1])
    for p in range(nv):
        cols = slice(p * slice_w, (p + 1) * slice_w)
        calls_o[:, cols] = samp_g[p, 0:2, :].astype(jnp.int32)
        share_o[:, cols] = samp_g[p, 2:3, :] * (samples_all / (nv * rows))

    @pl.when(y == 0)
    def _():
        drain(fin_o.at[1], fo_r.at[1])

    @pl.when(y == 1)
    def _():
        drain(fin_o.at[0], fo_r.at[0])
        drain(fin_o.at[1], fo_r.at[1])

    @pl.when(y < 2)
    def _():
        for h in range(2):
            for q in range(QUARTERS):
                ld_o[h * TILE : (h + 1) * TILE, q * qw : (q + 1) * qw] = fin_o[h, q]

    @pl.when(y >= 2)
    def _():
        @pl.when(b < nv - 1)
        def _():
            for h in range(2):
                drain(fin_n.at[h, pl.ds(0, ny - 1)], fn_r.at[h])
                drain(fin_p.at[h], fp_r.at[h])
            for h in range(2):
                for q in range(QUARTERS):
                    ld_o[h * TILE : (h + 1) * TILE, q * qw : (q + 1) * qw] = (
                        fin_n[h, q] + fin_p[h, q]
                    )

        @pl.when(b == nv - 1)
        def _():
            ld_o[...] = jnp.zeros_like(ld_o)

    drain(crit_z.at[pl.ds(0, nz - 1)], stat_s.at[0])
    drain(cnt_z.at[pl.ds(0, nz - 1)], stat_s.at[1])
    drain(crit_y.at[pl.ds(0, ny - 1)], stat_s.at[2])
    drain(cnt_y.at[pl.ds(0, ny - 1)], stat_s.at[3])
    drain(samp_r.at[pl.ds(0, nv - 1)], samp_ss.at[0])
    drain(samp_g.at[pl.ds(0, nv - 1)], samp_ss.at[1])

    def sent(u, carry):
        drain(yrecv.at[u], ys_sem.at[u])
        drain(zrecv.at[u], zs_sem.at[u])
        return carry

    lax.fori_loop(0, QUARTERS, sent, 0)

    @pl.when(y > 0)
    def _():
        o_copy().wait_send()

    @pl.when(b < nv - 1)
    def _():
        lax.fori_loop(QUARTERS, 2 * QUARTERS, sent, 0)
        to_next.wait_send()
        for c in range(QUARTERS):
            copy_p(c).wait_send()

            @pl.when(y != 2 + c // 2)
            def _():
                n_copy(c).wait_send()

    @pl.when(b > 0)
    def _():
        lax.fori_loop(2 * QUARTERS, 3 * QUARTERS, sent, 0)
        to_prev.wait_send()
        p_copy().wait_send()
        for c in range(QUARTERS):
            copy_n(c).wait_send()


def on_device(ny, nz, nv, genotypes, weights):
    rows, cols = genotypes.shape
    blocks = rows // TILE
    width, qw, slice_w = cols // PARTS, rows // QUARTERS, cols // nv
    half = PARTS // 2
    bf16 = jnp.bfloat16
    vmem = pl.BlockSpec(memory_space=pltpu.VMEM)
    dma = pltpu.SemaphoreType.DMA
    units = 3 * QUARTERS
    shapes = (
        ((1, rows), F32),
        ((1, rows), F32),
        ((4, rows), jnp.int32),
        ((2 * TILE, rows), F32),
        ((2, cols), jnp.int32),
        ((1, cols), F32),
    )
    mean, var, counts, ld, calls, share = pl.pallas_call(
        functools.partial(kernel, ny, nz, nv, cols * ny * nz),
        out_shape=[jax.ShapeDtypeStruct(s, t) for s, t in shapes],
        in_specs=[pl.BlockSpec(memory_space=pl.ANY), vmem],
        out_specs=[vmem] * len(shapes),
        scratch_shapes=[
            pltpu.VMEM((blocks, TILE, cols), jnp.int32),
            pltpu.VMEM((PARTS, 2, nz, 2, TILE, width), bf16),
            pltpu.VMEM((PARTS, blocks, TILE, width), bf16),
            pltpu.VMEM((QUARTERS, half, nz, TILE, width), bf16),
            pltpu.VMEM((QUARTERS, half, nz // 2, 2, TILE, width), bf16),
            pltpu.VMEM((TILE, cols), F32),
            pltpu.VMEM((TILE, cols), F32),
            pltpu.VMEM((3, blocks, TILE, LANES), F32),
            pltpu.VMEM((blocks, TILE, LANES), jnp.int32),
            pltpu.VMEM((8, cols), jnp.int32),
            pltpu.VMEM((8, cols), F32),
            pltpu.VMEM((nz, 4, rows), F32),
            pltpu.VMEM((ny, 4, rows), F32),
            pltpu.VMEM((nz, 4, rows), F32),
            pltpu.VMEM((ny, 4, rows), F32),
            pltpu.VMEM((3, 2, rows), F32),
            pltpu.VMEM((3, 2, 2, nz, 2, TILE, LANES), F32),
            pltpu.VMEM((nv, 4, slice_w), F32),
            pltpu.VMEM((nv, 4, slice_w), F32),
            pltpu.VMEM((nv, 4, slice_w), F32),
            pltpu.VMEM((rows, rows // 2), F32),
            pltpu.VMEM((units, ny, nz, TILE, qw), HALF),
            pltpu.VMEM((units, ny - 1, nz, TILE, qw), HALF),
            pltpu.VMEM((units, nz, TILE, qw), HALF),
            pltpu.VMEM((units, nz - 1, TILE, qw), HALF),
            pltpu.VMEM((units, TILE, qw), F32),
            pltpu.VMEM((2, QUARTERS, TILE, qw), F32),
            pltpu.VMEM((2, QUARTERS, TILE, qw), F32),
            pltpu.VMEM((2, QUARTERS, TILE, qw), F32),
            dma((8,)),
            dma((QUARTERS,)),
            dma((QUARTERS,)),
            dma((QUARTERS,)),
            dma((QUARTERS,)),
            dma((4,)),
            dma((4,)),
            dma((2,)),
            dma((2,)),
            dma((2,)),
            dma((2,)),
            dma((units,)),
            dma((units,)),
            dma((units,)),
            dma((units,)),
            dma((1,)),
            dma((2,)),
            dma((QUARTERS,)),
            dma((2,)),
            dma((1,)),
            dma((2,)),
        ],
        compiler_params=pltpu.CompilerParams(
            collective_id=0, has_side_effects=True, vmem_limit_bytes=60 * 2**20
        ),
    )(genotypes.reshape(blocks, TILE, cols), weights.reshape(1, cols))
    return (
        mean.reshape(rows),
        var.reshape(rows),
        counts,
        ld,
        calls,
        share.reshape(cols),
    )


def solution(mesh):
    ny = 4
    return jax.shard_map(
        functools.partial(on_device, ny, mesh.shape["samples"] // ny, mesh.shape["variants"]),
        mesh=mesh,
        in_specs=(P("variants", "samples"), P("samples")),
        out_specs=(
            P("variants"),
            P("variants"),
            P(None, "variants"),
            P("samples", "variants"),
            P(None, "samples"),
            P("samples"),
        ),
        check_vma=False,
    )
```

```python
import functools

import jax
import jax.numpy as jnp
from jax import lax
from jax.experimental import pallas as pl
from jax.experimental.pallas import tpu as pltpu
from jax.sharding import PartitionSpec as P

MESH = pl.DeviceIdType.MESH
LANES = 128
PARTS = 8
QUARTERS = 4
TILE = 16
HALF = jnp.int16
STEPS = 32000.0
F32 = jnp.float32
NT = (((1,), (1,)), ((), ()))


def drain(ref, sem):
    pltpu.make_async_copy(ref, ref, sem).wait()


def folded(value):
    return sum(value[:, i : i + LANES] for i in range(0, value.shape[1], LANES))


def coded(value):
    size = jnp.minimum(jnp.sqrt(jnp.abs(value)) * STEPS + 0.5, 32767.0).astype(jnp.int32)
    return jnp.where(value < 0.0, -size, size).astype(HALF)


def decoded(code):
    value = code.astype(jnp.int32).astype(F32)
    return value * jnp.abs(value)


def spread(value, width):
    return jnp.concatenate([value] * (width // LANES), axis=1)


def kernel(
    ny, nz, nv,
    g_hbm, w_ref,
    stat_o, ld_o, samp_o,
    gbuf, raw, scl, scl_n, scl_p, recv_n, recv_p, wide_w, root_w, moments, codes, col, squares,
    crit_z, crit_y, cnt_z, cnt_y, mf, bcast, samp_s, samp_r, samp_g, acc,
    ysend, yfar, ynear, zsend, zrecv, fin, fin_o, fin_n, fin_p,
    gsem, xs_n, xs_p, xr_n, xr_p, stat_s, stat_r, mf_s, mf_r, samp_ss, samp_rs,
    ya_s, ya_r, yb_s, yb_r, zs_sem, zr_sem, fo_s, fo_r, fn_s, fn_r, fp_s, fp_r,
):
    k, b = lax.axis_index("samples"), lax.axis_index("variants")
    y, z = k // nz, k % nz
    blocks = 4 * nz
    rows = blocks * TILE
    width = gbuf.shape[2] // PARTS
    half = PARTS // 2
    slice_w = gbuf.shape[2] // nv
    first, last = b == 0, b == nv - 1

    def at(ky, kz):
        return {"samples": ky * nz + kz}

    for part in range(8):
        group = pl.ds(part * (blocks // 8), blocks // 8)
        pltpu.make_async_copy(g_hbm.at[group], gbuf.at[group], gsem.at[part]).start()

    barrier = pltpu.get_barrier_semaphore()

    def greet(device):
        pl.semaphore_signal(barrier, inc=1, device_id=device, device_id_type=MESH)

    for d in range(1, ny):
        greet(at((y + d) % ny, z))
    for d in range(1, nz):
        greet(at(y, (z + d) % nz))
    for d in range(1, nv):
        greet({"variants": (b + d) % nv})

    @pl.when(b > 0)
    def _():
        for d in range(1, ny):
            greet({"samples": ((y + d) % ny) * nz + z, "variants": b - 1})

    @pl.when(b < nv - 1)
    def _():
        for d in range(1, ny):
            greet({"samples": ((y + d) % ny) * nz + z, "variants": b + 1})

    wide_w[...] = jnp.broadcast_to(w_ref[...], wide_w.shape)
    root_w[...] = jnp.sqrt(wide_w[...])
    col[...] = jnp.zeros_like(col)
    squares[...] = jnp.zeros_like(squares)

    def place(rb):
        return rb // (2 * nz), (rb // 2) % nz, rb % 2

    def first_pass(rb, carry):
        yr, zz, hh = place(rb)
        sum_w = jnp.zeros((TILE, LANES), F32)
        sum_1 = jnp.zeros((TILE, LANES), F32)
        sum_2 = jnp.zeros((TILE, LANES), F32)
        for kc in range(PARTS):
            cols = slice(kc * width, (kc + 1) * width)
            g = gbuf[rb, :, cols]
            gf = g.astype(F32)
            raw[kc, yr, zz, hh] = gf.astype(jnp.bfloat16)
            kept = jnp.where(g == 3, 0.0, wide_w[:, cols])
            once = kept * gf
            twice = once * gf
            sum_w += folded(kept)
            sum_1 += folded(once)
            sum_2 += folded(twice)
        moments[0, rb] = sum_w
        moments[1, rb] = sum_1
        moments[2, rb] = sum_2
        return carry

    def count_pass(rb, carry):
        sum_c = jnp.zeros((TILE, LANES), jnp.int32)
        for kc in range(PARTS):
            cols = slice(kc * width, (kc + 1) * width)
            g = gbuf[rb, :, cols]
            code = jnp.left_shift(jnp.ones_like(g), g * 8)
            col[:, cols] += code[:8] + code[8:]
            sum_c += folded(code)
        codes[rb] = sum_c
        return carry

    def copy_n(c):
        return pltpu.make_async_remote_copy(
            src_ref=raw.at[pl.ds(0, half), c // 2, :, c % 2],
            dst_ref=recv_n.at[c],
            send_sem=xs_n.at[c],
            recv_sem=xr_n.at[c],
            device_id={"variants": jnp.maximum(b - 1, 0)},
            device_id_type=MESH,
        )

    def copy_p(c):
        return pltpu.make_async_remote_copy(
            src_ref=raw.at[pl.ds(half, half), c // 2, pl.ds((c % 2) * (nz // 2), nz // 2)],
            dst_ref=recv_p.at[c],
            send_sem=xs_p.at[c],
            recv_sem=xr_p.at[c],
            device_id={"variants": jnp.minimum(b + 1, nv - 1)},
            device_id_type=MESH,
        )

    def wait_part(part):
        group = pl.ds(part * (blocks // 8), blocks // 8)
        pltpu.make_async_copy(g_hbm.at[group], gbuf.at[group], gsem.at[part]).wait()

    neighbours = jnp.where(b > 0, ny - 1, 0) + jnp.where(b < nv - 1, ny - 1, 0)
    for part in range(8):
        wait_part(part)
        lax.fori_loop(part * (blocks // 8), (part + 1) * (blocks // 8), first_pass, 0)

    def start_chunk(c):
        @pl.when(b < nv - 1)
        def _():
            copy_p(c).start()

        @pl.when(b > 0)
        def _():
            copy_n(c).start()

    def to_row(value):
        return jnp.sum(value.reshape(rows, LANES).T, axis=0, keepdims=True)

    def push(src, dst, i, device):
        return pltpu.make_async_remote_copy(
            src_ref=src,
            dst_ref=dst,
            send_sem=stat_s.at[i],
            recv_sem=stat_r.at[i],
            device_id=device,
            device_id_type=MESH,
        )

    for q in range(3):
        crit_z[z, q : q + 1, :] = to_row(moments[q])
    crit_z[z, 3:4, :] = jnp.zeros((1, rows), F32)
    pl.semaphore_wait(barrier, (ny - 1) + (nz - 1) + (nv - 1) + neighbours)
    for d in range(1, nz):
        push(crit_z.at[z], crit_z.at[z], 0, at(y, (z + d) % nz)).start()
    start_chunk(0)
    start_chunk(1)
    lax.fori_loop(0, blocks, count_pass, 0)
    fields = codes[...]
    for level in range(4):
        field = jnp.bitwise_and(jnp.right_shift(fields, 8 * level), 255)
        cnt_z[z, level : level + 1, :] = to_row(field.astype(F32))
    for d in range(1, nz):
        push(cnt_z.at[z], cnt_z.at[z], 1, at(y, (z + d) % nz)).start()

    drain(crit_z.at[pl.ds(0, nz - 1)], stat_r.at[0])
    crit_y[y] = sum(crit_z[i] for i in range(nz))
    for d in range(1, ny):
        push(crit_y.at[y], crit_y.at[y], 2, at((y + d) % ny, z)).start()
    start_chunk(2)
    drain(crit_y.at[pl.ds(0, ny - 1)], stat_r.at[2])
    total = sum(crit_y[i] for i in range(ny))
    w_sum, first_total, second_total = total[0:1], total[1:2], total[2:3]
    mean = first_total / w_sum
    var = (second_total - first_total * mean) / w_sum
    factor = 1.0 / jnp.sqrt(w_sum * (var + 1e-05))
    stat_o[0:1, :] = mean
    stat_o[1:2, :] = var
    stat_o[2:4, :] = jnp.zeros((2, rows), F32)
    mf[0, 0:1, :] = mean
    mf[0, 1:2, :] = factor

    def mf_copy(slot, target):
        return pltpu.make_async_remote_copy(
            src_ref=mf.at[0],
            dst_ref=mf.at[slot],
            send_sem=mf_s.at[slot - 1],
            recv_sem=mf_r.at[slot - 1],
            device_id={"variants": target},
            device_id_type=MESH,
        )

    to_prev = mf_copy(1, jnp.maximum(b - 1, 0))
    to_next = mf_copy(2, jnp.minimum(b + 1, nv - 1))

    @pl.when(b > 0)
    def _():
        to_prev.start()

    @pl.when(b < nv - 1)
    def _():
        to_next.start()

    start_chunk(3)

    def widen(slot):
        for q in range(2):
            tall = jnp.broadcast_to(mf[slot, q : q + 1, :], (LANES, rows)).T
            bcast[slot, q] = tall.reshape(2, nz, 2, TILE, LANES)

    def scaled(value, roots, mean_rows, factor_rows):
        x = value.astype(F32)
        out = (roots * (x - spread(mean_rows, width))) * spread(factor_rows, width)
        return jnp.where(x > 2.5, 0.0, out).astype(jnp.bfloat16)

    widen(0)

    drain(cnt_z.at[pl.ds(0, nz - 1)], stat_r.at[1])
    cnt_y[y] = sum(cnt_z[i] for i in range(nz))
    for d in range(1, ny):
        push(cnt_y.at[y], cnt_y.at[y], 3, at((y + d) % ny, z)).start()

    def second_pass(rb, carry):
        yr, zz, hh = place(rb)
        mean_rows, factor_rows = bcast[0, 0, yr, zz, hh], bcast[0, 1, yr, zz, hh]
        for kc in range(PARTS):
            cols = slice(kc * width, (kc + 1) * width)
            out = scaled(raw[kc, yr, zz, hh], root_w[:, cols], mean_rows, factor_rows)
            scl[pl.ds(pl.multiple_of(rb * TILE, TILE), TILE), cols] = out
        return carry

    def square_pass(rb, carry):
        for kc in range(PARTS):
            cols = slice(kc * width, (kc + 1) * width)
            wide = scl[pl.ds(pl.multiple_of(rb * TILE, TILE), TILE), cols].astype(F32)
            wide = wide * wide
            squares[:, cols] += wide[:8] + wide[8:]
        return carry

    lax.fori_loop(0, blocks, second_pass, 0)

    def samp_copy(i, src, dst, target):
        return pltpu.make_async_remote_copy(
            src_ref=src,
            dst_ref=dst,
            send_sem=samp_ss.at[i],
            recv_sem=samp_rs.at[i],
            device_id={"variants": target},
            device_id_type=MESH,
        )

    def per_sample():
        lax.fori_loop(0, blocks, square_pass, 0)
        packed = col[...]
        missing = jnp.sum(jnp.bitwise_and(jnp.right_shift(packed, 24), 255), axis=0, keepdims=True)
        het = jnp.sum(jnp.bitwise_and(jnp.right_shift(packed, 8), 255), axis=0, keepdims=True)
        called = (rows - missing).astype(F32)
        het = het.astype(F32)
        share = jnp.sum(squares[...], axis=0, keepdims=True)
        for p in range(nv):
            cols = slice(p * slice_w, (p + 1) * slice_w)
            samp_s[p, 0:1, :] = called[:, cols]
            samp_s[p, 1:2, :] = het[:, cols]
            samp_s[p, 2:3, :] = share[:, cols]
            samp_s[p, 3:4, :] = jnp.zeros((1, slice_w), F32)
        samp_r[b] = samp_s[b]
        for d in range(1, nv):
            target = (b + d) % nv
            samp_copy(0, samp_s.at[target], samp_r.at[b], target).start()

    up, down, across = (y + 1) % ny, (y + ny - 1) % ny, (y + 2) % ny
    lower, upper = pl.ds(0, nz // 2), pl.ds(nz // 2, nz // 2)

    def y_copy(src, dst, sems, target):
        return pltpu.make_async_remote_copy(
            src_ref=src,
            dst_ref=dst,
            send_sem=sems[0],
            recv_sem=sems[1],
            device_id=at(target, z),
            device_id_type=MESH,
        )

    def z_copy(u, d):
        target = (z + d) % nz
        return pltpu.make_async_remote_copy(
            src_ref=zsend.at[u, target],
            dst_ref=zrecv.at[u, d - 1],
            send_sem=zs_sem.at[u],
            recv_sem=zr_sem.at[u],
            device_id=at(y, target),
            device_id_type=MESH,
        )

    def y_start(u):
        sems = ya_s.at[u], ya_r.at[u]
        y_copy(ysend.at[u, across, lower], yfar.at[u, 0], sems, up).start()
        y_copy(ysend.at[u, across, upper], yfar.at[u, 1], sems, down).start()

    def y_direct(u):
        far, near = (ya_s.at[u], ya_r.at[u]), (yb_s.at[u], yb_r.at[u])
        y_copy(ysend.at[u, up], ynear.at[u, 0], near, up).start()
        y_copy(ysend.at[u, down], ynear.at[u, 1], near, down).start()
        y_copy(ysend.at[u, across, lower], yfar.at[u, 0], far, across).start()
        y_copy(ysend.at[u, across, upper], yfar.at[u, 1], far, across).start()

    def y_relay(u):
        drain(yfar.at[u], ya_r.at[u])
        sems = yb_s.at[u], yb_r.at[u]
        for slot, target, part in ((0, up, lower), (1, down, upper)):
            both = decoded(ysend[u, target, part]) + decoded(yfar[u, slot])
            ysend[u, target, part] = coded(both * (1.0 / STEPS**2))
            y_copy(ysend.at[u, target], ynear.at[u, slot], sems, target).start()

    def z_start(u, part):
        zsend[u] = coded(part * (1.0 / STEPS**2))
        for d in range(1, nz):
            z_copy(u, d).start()

    def y_fold_all(u):
        drain(ynear.at[u], yb_r.at[u])
        drain(yfar.at[u], ya_r.at[u])
        part = decoded(ysend[u, y]) + decoded(ynear[u, 0]) + decoded(ynear[u, 1])
        z_start(u, part + decoded(yfar[u]).reshape(nz, TILE, qw))

    def y_fold(u):
        drain(ynear.at[u], yb_r.at[u])
        z_start(u, decoded(ysend[u, y]) + decoded(ynear[u, 0]) + decoded(ynear[u, 1]))

    def z_fold(u):
        drain(zrecv.at[u], zr_sem.at[u])
        part = decoded(zsend[u, z])
        for d in range(nz - 1):
            part = part + decoded(zrecv[u, d])
        fin[u] = part * (1.0 / STEPS**2)

    qw = rows // QUARTERS

    def group_rows(value, u):
        value = coded(value).reshape(2, nz, 2, TILE, qw)
        for yr in range(2):
            for hh in range(2):
                ysend[u, 2 * yr + hh] = value[yr, :, hh]

    for pair in range(2):
        with jax.named_scope("own_dot"):
            acc[...] = lax.dot_general(
                scl[...],
                scl[pair * (rows // 2) : (pair + 1) * (rows // 2)],
                NT,
                preferred_element_type=F32,
            )
        for j in range(2):
            group_rows(acc[:, j * qw : (j + 1) * qw], 2 * pair + j)
            y_start(2 * pair + j)

    @pl.when(b < nv - 1)
    def _():
        to_prev.wait_recv()
        widen(1)

    @pl.when(b > 0)
    def _():
        to_next.wait_recv()
        widen(2)

    def y_begin(c, u):
        @pl.when(c < QUARTERS - 1)
        def _():
            y_start(u)

        @pl.when(c == QUARTERS - 1)
        def _():
            y_direct(u)

    def chunk_n(c):
        copy_n(c).wait_recv()
        for kc in range(half):
            roots = root_w[:, kc * width : (kc + 1) * width]
            for zz in range(nz):
                scl_n[zz * TILE : (zz + 1) * TILE, kc * width : (kc + 1) * width] = scaled(
                    recv_n[c, kc, zz],
                    roots,
                    bcast[1, 0, c // 2, zz, c % 2],
                    bcast[1, 1, c // 2, zz, c % 2],
                )
        out = lax.dot_general(
            scl_n[...], scl[:, : half * width], NT, preferred_element_type=F32
        )
        out = coded(out)
        for q in range(QUARTERS):
            ysend[4 + c, q] = out[:, q * qw : (q + 1) * qw].reshape(nz, TILE, qw)
        y_begin(c, 4 + c)

    def chunk_p(c):
        copy_p(c).wait_recv()
        for kc in range(half):
            roots = root_w[:, (half + kc) * width : (half + kc + 1) * width]
            for zz in range(nz // 2):
                for hh in range(2):
                    spot = (c // 2, (c % 2) * (nz // 2) + zz, hh)
                    start = (2 * zz + hh) * TILE
                    scl_p[start : start + TILE, kc * width : (kc + 1) * width] = scaled(
                        recv_p[c, kc, zz, hh], roots, bcast[(2, 0, *spot)], bcast[(2, 1, *spot)]
                    )
        out = lax.dot_general(
            scl[:, half * width :], scl_p[...], NT, preferred_element_type=F32
        )
        group_rows(out, 8 + c)
        y_begin(c, 8 + c)

    def n_copy(c):
        return pltpu.make_async_remote_copy(
            src_ref=fin.at[4 + c],
            dst_ref=fin_n.at[c % 2, y],
            send_sem=fn_s.at[c],
            recv_sem=fn_r.at[c % 2],
            device_id=at(2 + c // 2, z),
            device_id_type=MESH,
        )

    def o_copy():
        return pltpu.make_async_remote_copy(
            src_ref=fin.at[pl.ds(0, QUARTERS)],
            dst_ref=fin_o.at[y % 2],
            send_sem=fo_s.at[0],
            recv_sem=fo_r.at[y % 2],
            device_id=at(y // 2, z),
            device_id_type=MESH,
        )

    def p_copy():
        return pltpu.make_async_remote_copy(
            src_ref=fin.at[pl.ds(8, QUARTERS)],
            dst_ref=fin_p.at[y % 2],
            send_sem=fp_s.at[0],
            recv_sem=fp_r.at[y % 2],
            device_id={"samples": (2 + y // 2) * nz + z, "variants": jnp.maximum(b - 1, 0)},
            device_id_type=MESH,
        )

    def n_final(c):
        owner = 2 + c // 2

        @pl.when(y == owner)
        def _():
            fin_n[c % 2, y] = fin[4 + c]

        @pl.when(y != owner)
        def _():
            n_copy(c).start()

    def step(c, carry):
        @pl.when(c < QUARTERS)
        def _():
            @pl.when(b < nv - 1)
            def _():
                chunk_n(c)

            @pl.when(b > 0)
            def _():
                chunk_p(c)

        def both(at_c, action):
            @pl.when(b < nv - 1)
            def _():
                action(QUARTERS + at_c)

            @pl.when(b > 0)
            def _():
                action(2 * QUARTERS + at_c)

        def own_units(action):
            for u in range(QUARTERS):
                action(u)

        @pl.when(c == 0)
        def _():
            own_units(y_relay)

        @pl.when(c == 1)
        def _():
            both(0, y_relay)

        @pl.when(c == 2)
        def _():
            own_units(y_fold)
            both(1, y_relay)

        @pl.when(c == 3)
        def _():
            per_sample()
            both(2, y_relay)
            both(0, y_fold)
            both(1, y_fold)

        @pl.when(c == 4)
        def _():
            both(3, y_fold_all)
            both(2, y_fold)
            own_units(z_fold)

            @pl.when(y == 0)
            def _():
                fin_o[0] = fin[0:QUARTERS]

            @pl.when(y > 0)
            def _():
                o_copy().start()

        @pl.when(c == 6)
        def _():
            drain(samp_r.at[pl.ds(0, nv - 1)], samp_rs.at[0])
            samp_g[b] = sum(samp_r[p] for p in range(nv))
            for d in range(1, nv):
                samp_copy(1, samp_g.at[b], samp_g.at[b], (b + d) % nv).start()

        @pl.when(c > QUARTERS)
        def _():
            both(c - QUARTERS - 1, z_fold)

            @pl.when(b < nv - 1)
            def _():
                n_final(c - QUARTERS - 1)

        return carry

    lax.fori_loop(0, 2 * QUARTERS + 1, step, 0)

    @pl.when(b > 0)
    def _():
        p_copy().start()

    drain(cnt_y.at[pl.ds(0, ny - 1)], stat_r.at[3])
    stat_o[4:8, :] = sum(cnt_y[i] for i in range(ny))
    drain(samp_g.at[pl.ds(0, nv - 1)], samp_rs.at[1])
    samp_o[...] = samp_g[...]

    @pl.when(y == 0)
    def _():
        drain(fin_o.at[1], fo_r.at[1])

    @pl.when(y == 1)
    def _():
        drain(fin_o.at[0], fo_r.at[0])
        drain(fin_o.at[1], fo_r.at[1])

    @pl.when(y < 2)
    def _():
        for h in range(2):
            for q in range(QUARTERS):
                ld_o[h * TILE : (h + 1) * TILE, q * qw : (q + 1) * qw] = fin_o[h, q]

    @pl.when(y >= 2)
    def _():
        @pl.when(b < nv - 1)
        def _():
            for h in range(2):
                drain(fin_n.at[h, pl.ds(0, ny - 1)], fn_r.at[h])
                drain(fin_p.at[h], fp_r.at[h])
            for h in range(2):
                for q in range(QUARTERS):
                    ld_o[h * TILE : (h + 1) * TILE, q * qw : (q + 1) * qw] = (
                        fin_n[h, q] + fin_p[h, q]
                    )

        @pl.when(b == nv - 1)
        def _():
            ld_o[...] = jnp.zeros_like(ld_o)

    drain(crit_z.at[pl.ds(0, nz - 1)], stat_s.at[0])
    drain(cnt_z.at[pl.ds(0, nz - 1)], stat_s.at[1])
    drain(crit_y.at[pl.ds(0, ny - 1)], stat_s.at[2])
    drain(cnt_y.at[pl.ds(0, ny - 1)], stat_s.at[3])
    drain(samp_r.at[pl.ds(0, nv - 1)], samp_ss.at[0])
    drain(samp_g.at[pl.ds(0, nv - 1)], samp_ss.at[1])

    def sent(u, carry):
        drain(yfar.at[u], ya_s.at[u])
        drain(ynear.at[u], yb_s.at[u])
        drain(zrecv.at[u], zs_sem.at[u])
        return carry

    lax.fori_loop(0, QUARTERS, sent, 0)

    @pl.when(y > 0)
    def _():
        o_copy().wait_send()

    @pl.when(b < nv - 1)
    def _():
        lax.fori_loop(QUARTERS, 2 * QUARTERS, sent, 0)
        to_next.wait_send()
        for c in range(QUARTERS):
            copy_p(c).wait_send()

            @pl.when(y != 2 + c // 2)
            def _():
                n_copy(c).wait_send()

    @pl.when(b > 0)
    def _():
        lax.fori_loop(2 * QUARTERS, 3 * QUARTERS, sent, 0)
        to_prev.wait_send()
        p_copy().wait_send()
        for c in range(QUARTERS):
            copy_n(c).wait_send()


def deliver(ratio, stat_ref, ld_ref, samp_ref, mean_o, var_o, count_o, ld_o, calls_o, share_o):
    mean_o[...] = stat_ref[0:1, :]
    var_o[...] = stat_ref[1:2, :]
    count_o[...] = stat_ref[4:8, :].astype(jnp.int32)
    ld_o[...] = ld_ref[...]
    slice_w = samp_ref.shape[2]
    for p in range(samp_ref.shape[0]):
        cols = slice(p * slice_w, (p + 1) * slice_w)
        calls_o[:, cols] = samp_ref[p, 0:2, :].astype(jnp.int32)
        share_o[:, cols] = samp_ref[p, 2:3, :] * ratio


def on_device(ny, nz, nv, genotypes, weights):
    rows, cols = genotypes.shape
    blocks = rows // TILE
    width, qw, slice_w = cols // PARTS, rows // QUARTERS, cols // nv
    half = PARTS // 2
    bf16 = jnp.bfloat16
    vmem = pl.BlockSpec(memory_space=pltpu.VMEM)
    dma = pltpu.SemaphoreType.DMA
    units = 3 * QUARTERS
    shapes = (((8, rows), F32), ((2 * TILE, rows), F32), ((nv, 4, slice_w), F32))
    held = pl.pallas_call(
        functools.partial(kernel, ny, nz, nv),
        out_shape=[jax.ShapeDtypeStruct(s, t) for s, t in shapes],
        in_specs=[pl.BlockSpec(memory_space=pl.ANY), vmem],
        out_specs=[vmem] * len(shapes),
        scratch_shapes=[
            pltpu.VMEM((blocks, TILE, cols), jnp.int32),
            pltpu.VMEM((PARTS, 2, nz, 2, TILE, width), bf16),
            pltpu.VMEM((rows, cols), bf16),
            pltpu.VMEM((nz * TILE, half * width), bf16),
            pltpu.VMEM((qw, half * width), bf16),
            pltpu.VMEM((QUARTERS, half, nz, TILE, width), bf16),
            pltpu.VMEM((QUARTERS, half, nz // 2, 2, TILE, width), bf16),
            pltpu.VMEM((TILE, cols), F32),
            pltpu.VMEM((TILE, cols), F32),
            pltpu.VMEM((3, blocks, TILE, LANES), F32),
            pltpu.VMEM((blocks, TILE, LANES), jnp.int32),
            pltpu.VMEM((8, cols), jnp.int32),
            pltpu.VMEM((8, cols), F32),
            pltpu.VMEM((nz, 4, rows), F32),
            pltpu.VMEM((ny, 4, rows), F32),
            pltpu.VMEM((nz, 4, rows), F32),
            pltpu.VMEM((ny, 4, rows), F32),
            pltpu.VMEM((3, 2, rows), F32),
            pltpu.VMEM((3, 2, 2, nz, 2, TILE, LANES), F32),
            pltpu.VMEM((nv, 4, slice_w), F32),
            pltpu.VMEM((nv, 4, slice_w), F32),
            pltpu.VMEM((nv, 4, slice_w), F32),
            pltpu.VMEM((rows, rows // 2), F32),
            pltpu.VMEM((units, ny, nz, TILE, qw), HALF),
            pltpu.VMEM((units, 2, nz // 2, TILE, qw), HALF),
            pltpu.VMEM((units, 2, nz, TILE, qw), HALF),
            pltpu.VMEM((units, nz, TILE, qw), HALF),
            pltpu.VMEM((units, nz - 1, TILE, qw), HALF),
            pltpu.VMEM((units, TILE, qw), F32),
            pltpu.VMEM((2, QUARTERS, TILE, qw), F32),
            pltpu.VMEM((2, QUARTERS, TILE, qw), F32),
            pltpu.VMEM((2, QUARTERS, TILE, qw), F32),
            dma((8,)),
            dma((QUARTERS,)),
            dma((QUARTERS,)),
            dma((QUARTERS,)),
            dma((QUARTERS,)),
            dma((4,)),
            dma((4,)),
            dma((2,)),
            dma((2,)),
            dma((2,)),
            dma((2,)),
            dma((units,)),
            dma((units,)),
            dma((units,)),
            dma((units,)),
            dma((units,)),
            dma((units,)),
            dma((1,)),
            dma((2,)),
            dma((QUARTERS,)),
            dma((2,)),
            dma((1,)),
            dma((2,)),
        ],
        compiler_params=pltpu.CompilerParams(
            collective_id=0, has_side_effects=True, vmem_limit_bytes=60 * 2**20
        ),
    )(genotypes.reshape(blocks, TILE, cols), weights.reshape(1, cols))
    shapes = (
        ((1, rows), F32),
        ((1, rows), F32),
        ((4, rows), jnp.int32),
        ((2 * TILE, rows), F32),
        ((2, cols), jnp.int32),
        ((1, cols), F32),
    )
    mean, var, counts, ld, calls, share = pl.pallas_call(
        functools.partial(deliver, ny * nz * cols / (nv * rows)),
        out_shape=[jax.ShapeDtypeStruct(s, t) for s, t in shapes],
        in_specs=[vmem] * 3,
        out_specs=[vmem] * len(shapes),
    )(*held)
    return (
        mean.reshape(rows),
        var.reshape(rows),
        counts,
        ld,
        calls,
        share.reshape(cols),
    )


def solution(mesh):
    ny = 4
    return jax.shard_map(
        functools.partial(on_device, ny, mesh.shape["samples"] // ny, mesh.shape["variants"]),
        mesh=mesh,
        in_specs=(P("variants", "samples"), P("samples")),
        out_specs=(
            P("variants"),
            P("variants"),
            P(None, "variants"),
            P("samples", "variants"),
            P(None, "samples"),
            P("samples"),
        ),
        check_vma=False,
    )
```

```python
import functools

import jax
import jax.numpy as jnp
from jax import lax
from jax.experimental import pallas as pl
from jax.experimental.pallas import tpu as pltpu
from jax.sharding import PartitionSpec as P

MESH = pl.DeviceIdType.MESH
LANES = 128
PARTS = 8
QUARTERS = 4
TILE = 16
HALF = jnp.int16
STEPS = 32000.0
F32 = jnp.float32
NT = (((1,), (1,)), ((), ()))
NN = (((1,), (0,)), ((), ()))


def drain(ref, sem):
    pltpu.make_async_copy(ref, ref, sem).wait()


def folded(value):
    return sum(value[:, i : i + LANES] for i in range(0, value.shape[1], LANES))


def coded(value):
    size = jnp.minimum(jnp.sqrt(jnp.abs(value)) * STEPS + 0.5, 32767.0).astype(jnp.int32)
    return jnp.where(value < 0.0, -size, size).astype(HALF)


def decoded(code):
    value = code.astype(jnp.int32).astype(F32)
    return value * jnp.abs(value)


def spread(value, width):
    return jnp.concatenate([value] * (width // LANES), axis=1)


def kernel(
    ny, nz, nv,
    g_hbm, w_ref,
    stat_o, ld_o, samp_o,
    gbuf, raw, scl, scl_t, scl_n, scl_p, acc_n, acc_m, recv_q, recv_n, recv_p, wide_w, root_w, moments, codes, col, squares,
    crit_z, crit_y, cnt_z, cnt_y, mf, bcast, samp_s, samp_r, samp_g, acc,
    ysend, yfar, ynear, zsend, zrecv, fin, fin_o, fin_n, fin_p,
    gsem, xs_q, xr_q, xs_n, xs_p, xr_n, xr_p, stat_s, stat_r, mf_s, mf_r, samp_ss, samp_rs,
    ya_s, ya_r, yb_s, yb_r, zs_sem, zr_sem, fo_s, fo_r, fn_s, fn_r, fp_s, fp_r,
):
    k, b = lax.axis_index("samples"), lax.axis_index("variants")
    y, z = k // nz, k % nz
    blocks = 4 * nz
    rows = blocks * TILE
    width = gbuf.shape[2] // PARTS
    half = PARTS // 2
    slice_w = gbuf.shape[2] // nv
    first, last = b == 0, b == nv - 1

    def at(ky, kz):
        return {"samples": ky * nz + kz}

    for part in range(8):
        group = pl.ds(part * (blocks // 8), blocks // 8)
        pltpu.make_async_copy(g_hbm.at[group], gbuf.at[group], gsem.at[part]).start()

    barrier = pltpu.get_barrier_semaphore()

    def greet(device):
        pl.semaphore_signal(barrier, inc=1, device_id=device, device_id_type=MESH)

    for d in range(1, ny):
        greet(at((y + d) % ny, z))
    for d in range(1, nz):
        greet(at(y, (z + d) % nz))
    for d in range(1, nv):
        greet({"variants": (b + d) % nv})

    @pl.when(b > 0)
    def _():
        for d in range(1, ny):
            greet({"samples": ((y + d) % ny) * nz + z, "variants": b - 1})

    @pl.when(b < nv - 1)
    def _():
        for d in range(1, ny):
            greet({"samples": ((y + d) % ny) * nz + z, "variants": b + 1})

    wide_w[...] = jnp.broadcast_to(w_ref[...], wide_w.shape)
    root_w[...] = jnp.sqrt(wide_w[...])
    col[...] = jnp.zeros_like(col)
    squares[...] = jnp.zeros_like(squares)

    def place(rb):
        return rb // (2 * nz), (rb // 2) % nz, rb % 2

    def first_pass(rb, carry):
        yr, zz, hh = place(rb)
        sum_w = jnp.zeros((TILE, LANES), F32)
        sum_1 = jnp.zeros((TILE, LANES), F32)
        sum_2 = jnp.zeros((TILE, LANES), F32)
        for kc in range(PARTS):
            cols = slice(kc * width, (kc + 1) * width)
            g = gbuf[rb, :, cols]
            gf = g.astype(F32)
            raw[kc, yr, zz, hh] = gf.astype(jnp.bfloat16)
            kept = jnp.where(g == 3, 0.0, wide_w[:, cols])
            once = kept * gf
            twice = once * gf
            sum_w += folded(kept)
            sum_1 += folded(once)
            sum_2 += folded(twice)
        moments[0, rb] = sum_w
        moments[1, rb] = sum_1
        moments[2, rb] = sum_2
        return carry

    def count_pass(rb, carry):
        sum_c = jnp.zeros((TILE, LANES), jnp.int32)
        for kc in range(PARTS):
            cols = slice(kc * width, (kc + 1) * width)
            g = gbuf[rb, :, cols]
            code = jnp.left_shift(jnp.ones_like(g), g * 8)
            col[:, cols] += code[:8] + code[8:]
            sum_c += folded(code)
        codes[rb] = sum_c
        return carry

    odd = b % 2

    def copy_n(c):
        return pltpu.make_async_remote_copy(
            src_ref=raw.at[
                pl.ds(odd * (c % 2) * half, half),
                (1 - odd) * (c // 2),
                :,
                odd * (c // 2) + (1 - odd) * (c % 2),
            ],
            dst_ref=recv_n.at[c],
            send_sem=xs_n.at[c],
            recv_sem=xr_n.at[c],
            device_id={"variants": jnp.maximum(b - 1, 0)},
            device_id_type=MESH,
        )

    def copy_rows(c, base, dst, send_sems, recv_sems):
        return pltpu.make_async_remote_copy(
            src_ref=raw.at[pl.ds(base, half), c // 2, pl.ds((c % 2) * (nz // 2), nz // 2)],
            dst_ref=dst.at[c],
            send_sem=send_sems.at[c],
            recv_sem=recv_sems.at[c],
            device_id={"variants": jnp.minimum(b + 1, nv - 1)},
            device_id_type=MESH,
        )

    def copy_p(c):
        return copy_rows(c, half, recv_p, xs_p, xr_p)

    def copy_q(c):
        return copy_rows(c, 0, recv_q, xs_q, xr_q)

    def wait_part(part):
        group = pl.ds(part * (blocks // 8), blocks // 8)
        pltpu.make_async_copy(g_hbm.at[group], gbuf.at[group], gsem.at[part]).wait()

    neighbours = jnp.where(b > 0, ny - 1, 0) + jnp.where(b < nv - 1, ny - 1, 0)
    for part in range(8):
        wait_part(part)
        lax.fori_loop(part * (blocks // 8), (part + 1) * (blocks // 8), first_pass, 0)

    def start_chunk(c):
        @pl.when(b < nv - 1)
        def _():
            copy_p(c).start()

        @pl.when(odd == 0)
        def _():
            copy_q(c).start()

        @pl.when(b > 0)
        def _():
            copy_n(c).start()

    def to_row(value):
        return jnp.sum(value.reshape(rows, LANES).T, axis=0, keepdims=True)

    def push(src, dst, i, device):
        return pltpu.make_async_remote_copy(
            src_ref=src,
            dst_ref=dst,
            send_sem=stat_s.at[i],
            recv_sem=stat_r.at[i],
            device_id=device,
            device_id_type=MESH,
        )

    for q in range(3):
        crit_z[z, q : q + 1, :] = to_row(moments[q])
    crit_z[z, 3:4, :] = jnp.zeros((1, rows), F32)
    pl.semaphore_wait(barrier, (ny - 1) + (nz - 1) + (nv - 1) + neighbours)
    for d in range(1, nz):
        push(crit_z.at[z], crit_z.at[z], 0, at(y, (z + d) % nz)).start()
    start_chunk(0)
    start_chunk(1)
    lax.fori_loop(0, blocks, count_pass, 0)
    fields = codes[...]
    for level in range(4):
        field = jnp.bitwise_and(jnp.right_shift(fields, 8 * level), 255)
        cnt_z[z, level : level + 1, :] = to_row(field.astype(F32))
    for d in range(1, nz):
        push(cnt_z.at[z], cnt_z.at[z], 1, at(y, (z + d) % nz)).start()

    drain(crit_z.at[pl.ds(0, nz - 1)], stat_r.at[0])
    crit_y[y] = sum(crit_z[i] for i in range(nz))
    for d in range(1, ny):
        push(crit_y.at[y], crit_y.at[y], 2, at((y + d) % ny, z)).start()
    drain(crit_y.at[pl.ds(0, ny - 1)], stat_r.at[2])
    total = sum(crit_y[i] for i in range(ny))
    w_sum, first_total, second_total = total[0:1], total[1:2], total[2:3]
    mean = first_total / w_sum
    var = (second_total - first_total * mean) / w_sum
    factor = 1.0 / jnp.sqrt(w_sum * (var + 1e-05))
    stat_o[0:1, :] = mean
    stat_o[1:2, :] = var
    stat_o[2:4, :] = jnp.zeros((2, rows), F32)
    mf[0, 0:1, :] = mean
    mf[0, 1:2, :] = factor

    def mf_copy(slot, target):
        return pltpu.make_async_remote_copy(
            src_ref=mf.at[0],
            dst_ref=mf.at[slot],
            send_sem=mf_s.at[slot - 1],
            recv_sem=mf_r.at[slot - 1],
            device_id={"variants": target},
            device_id_type=MESH,
        )

    to_prev = mf_copy(1, jnp.maximum(b - 1, 0))
    to_next = mf_copy(2, jnp.minimum(b + 1, nv - 1))

    @pl.when(b > 0)
    def _():
        to_prev.start()

    @pl.when(b < nv - 1)
    def _():
        to_next.start()

    start_chunk(2)
    start_chunk(3)

    def widen(slot):
        for q in range(2):
            tall = jnp.broadcast_to(mf[slot, q : q + 1, :], (LANES, rows)).T
            bcast[slot, q] = tall.reshape(2, nz, 2, TILE, LANES)

    def scaled(value, roots, mean_rows, factor_rows):
        x = value.astype(F32)
        out = (roots * (x - spread(mean_rows, width))) * spread(factor_rows, width)
        return jnp.where(x > 2.5, 0.0, out).astype(jnp.bfloat16)

    widen(0)

    drain(cnt_z.at[pl.ds(0, nz - 1)], stat_r.at[1])
    cnt_y[y] = sum(cnt_z[i] for i in range(nz))
    for d in range(1, ny):
        push(cnt_y.at[y], cnt_y.at[y], 3, at((y + d) % ny, z)).start()

    def second_pass(rb, carry):
        yr, zz, hh = place(rb)
        mean_rows, factor_rows = bcast[0, 0, yr, zz, hh], bcast[0, 1, yr, zz, hh]
        for kc in range(PARTS):
            cols = slice(kc * width, (kc + 1) * width)
            out = scaled(raw[kc, yr, zz, hh], root_w[:, cols], mean_rows, factor_rows)
            scl[pl.ds(pl.multiple_of(rb * TILE, TILE), TILE), cols] = out
        return carry

    def square_pass(rb, carry):
        for kc in range(PARTS):
            cols = slice(kc * width, (kc + 1) * width)
            wide = scl[pl.ds(pl.multiple_of(rb * TILE, TILE), TILE), cols].astype(F32)
            wide = wide * wide
            squares[:, cols] += wide[:8] + wide[8:]
        return carry

    lax.fori_loop(0, blocks, second_pass, 0)

    def samp_copy(i, src, dst, target):
        return pltpu.make_async_remote_copy(
            src_ref=src,
            dst_ref=dst,
            send_sem=samp_ss.at[i],
            recv_sem=samp_rs.at[i],
            device_id={"variants": target},
            device_id_type=MESH,
        )

    def per_sample():
        lax.fori_loop(0, blocks, square_pass, 0)
        packed = col[...]
        missing = jnp.sum(jnp.bitwise_and(jnp.right_shift(packed, 24), 255), axis=0, keepdims=True)
        het = jnp.sum(jnp.bitwise_and(jnp.right_shift(packed, 8), 255), axis=0, keepdims=True)
        called = (rows - missing).astype(F32)
        het = het.astype(F32)
        share = jnp.sum(squares[...], axis=0, keepdims=True)
        for p in range(nv):
            cols = slice(p * slice_w, (p + 1) * slice_w)
            samp_s[p, 0:1, :] = called[:, cols]
            samp_s[p, 1:2, :] = het[:, cols]
            samp_s[p, 2:3, :] = share[:, cols]
            samp_s[p, 3:4, :] = jnp.zeros((1, slice_w), F32)
        samp_r[b] = samp_s[b]
        for d in range(1, nv):
            target = (b + d) % nv
            samp_copy(0, samp_s.at[target], samp_r.at[b], target).start()

    up, down, across = (y + 1) % ny, (y + ny - 1) % ny, (y + 2) % ny
    lower, upper = pl.ds(0, nz // 2), pl.ds(nz // 2, nz // 2)

    def y_copy(src, dst, sems, target):
        return pltpu.make_async_remote_copy(
            src_ref=src,
            dst_ref=dst,
            send_sem=sems[0],
            recv_sem=sems[1],
            device_id=at(target, z),
            device_id_type=MESH,
        )

    def z_copy(u, d):
        target = (z + d) % nz
        return pltpu.make_async_remote_copy(
            src_ref=zsend.at[u, target],
            dst_ref=zrecv.at[u, d - 1],
            send_sem=zs_sem.at[u],
            recv_sem=zr_sem.at[u],
            device_id=at(y, target),
            device_id_type=MESH,
        )

    def y_start(u):
        sems = ya_s.at[u], ya_r.at[u]
        y_copy(ysend.at[u, across, lower], yfar.at[u, 0], sems, up).start()
        y_copy(ysend.at[u, across, upper], yfar.at[u, 1], sems, down).start()

    def y_direct(u):
        far, near = (ya_s.at[u], ya_r.at[u]), (yb_s.at[u], yb_r.at[u])
        y_copy(ysend.at[u, up], ynear.at[u, 0], near, up).start()
        y_copy(ysend.at[u, down], ynear.at[u, 1], near, down).start()
        y_copy(ysend.at[u, across, lower], yfar.at[u, 0], far, across).start()
        y_copy(ysend.at[u, across, upper], yfar.at[u, 1], far, across).start()

    def y_relay(u):
        drain(yfar.at[u], ya_r.at[u])
        sems = yb_s.at[u], yb_r.at[u]
        for slot, target, part in ((0, up, lower), (1, down, upper)):
            both = decoded(ysend[u, target, part]) + decoded(yfar[u, slot])
            ysend[u, target, part] = coded(both * (1.0 / STEPS**2))
            y_copy(ysend.at[u, target], ynear.at[u, slot], sems, target).start()

    def z_start(u, part):
        zsend[u] = coded(part * (1.0 / STEPS**2))
        for d in range(1, nz):
            z_copy(u, d).start()

    def y_fold_all(u):
        drain(ynear.at[u], yb_r.at[u])
        drain(yfar.at[u], ya_r.at[u])
        part = decoded(ysend[u, y]) + decoded(ynear[u, 0]) + decoded(ynear[u, 1])
        z_start(u, part + decoded(yfar[u]).reshape(nz, TILE, qw))

    def y_fold(u):
        drain(ynear.at[u], yb_r.at[u])
        z_start(u, decoded(ysend[u, y]) + decoded(ynear[u, 0]) + decoded(ynear[u, 1]))

    def z_fold(u):
        drain(zrecv.at[u], zr_sem.at[u])
        part = decoded(zsend[u, z])
        for d in range(nz - 1):
            part = part + decoded(zrecv[u, d])
        fin[u] = part * (1.0 / STEPS**2)

    qw = rows // QUARTERS

    def group_rows(value, u):
        value = coded(value).reshape(2, nz, 2, TILE, qw)
        for yr in range(2):
            for hh in range(2):
                ysend[u, 2 * yr + hh] = value[yr, :, hh]

    for pair in range(2):
        with jax.named_scope("own_dot"):
            if pair == 0:
                acc[...] = lax.dot_general(
                    scl[...], scl[: rows // 2], NT, preferred_element_type=F32
                )
            else:
                acc[: rows // 2] = acc[rows // 2 :].T
                acc[rows // 2 :] = lax.dot_general(
                    scl[rows // 2 :], scl[rows // 2 :], NT, preferred_element_type=F32
                )
        for j in range(2):
            group_rows(acc[:, j * qw : (j + 1) * qw], 2 * pair + j)
            y_start(2 * pair + j)

    @pl.when(b < nv - 1)
    def _():
        with jax.named_scope("turn"):
            scl_t[: half * width] = scl[:, : half * width].T

            @pl.when(odd == 0)
            def _():
                scl_t[half * width :] = scl[:, half * width :].T

        to_prev.wait_recv()
        widen(1)

    @pl.when(b > 0)
    def _():
        to_next.wait_recv()
        widen(2)

    def y_begin(c, u):
        @pl.when(c < QUARTERS - 2)
        def _():
            y_start(u)

        @pl.when(c >= QUARTERS - 2)
        def _():
            y_direct(u)

    def chunk_n(c):
        copy_n(c).wait_recv()
        side = (1 - odd) * (c % 2)
        yr, hh = odd * (c // 2), odd * (c % 2) + (1 - odd) * (c // 2)
        base = pl.multiple_of(side * half * width, half * width)
        for kc in range(half):
            roots = root_w[:, pl.ds(pl.multiple_of(base + kc * width, width), width)]
            for zz in range(nz):
                scl_n[zz * TILE : (zz + 1) * TILE, kc * width : (kc + 1) * width] = scaled(
                    recv_n[c, kc, zz], roots, bcast[1, 0, yr, zz, hh], bcast[1, 1, yr, zz, hh]
                )
        acc_n[...] = lax.dot_general(
            scl_n[...], scl_t[pl.ds(base, half * width)], NN, preferred_element_type=F32
        )

    def pack_n(c, u, out):
        out = coded(out)
        for q in range(QUARTERS):
            ysend[u, q] = out[:, q * qw : (q + 1) * qw].reshape(nz, TILE, qw)
        y_begin(c, u)

    def turn_p(c, buf, base):
        for kc in range(half):
            cols = slice((base + kc) * width, (base + kc + 1) * width)
            roots = root_w[:, cols]
            for zz in range(nz // 2):
                for hh in range(2):
                    spot = (c // 2, (c % 2) * (nz // 2) + zz, hh)
                    start = (2 * zz + hh) * TILE
                    scl_p[start : start + TILE, cols] = scaled(
                        buf[c, kc, zz, hh], roots, bcast[(2, 0, *spot)], bcast[(2, 1, *spot)]
                    )

    def chunk_p(c):
        copy_p(c).wait_recv()
        turn_p(c, recv_p, half)
        out = lax.dot_general(
            scl[:, half * width :], scl_p[:, half * width :], NT, preferred_element_type=F32
        )
        group_rows(out, 8 + c)
        y_begin(c, 8 + c)

    def chunk_q(c):
        copy_p(c).wait_recv()
        turn_p(c, recv_p, half)
        copy_q(c).wait_recv()
        turn_p(c, recv_q, 0)
        out = lax.dot_general(
            scl[rows // 2 :], scl_p[...], NT, preferred_element_type=F32
        )
        out = coded(out).reshape(nz, 2, TILE, qw)
        for hh in range(2):
            ysend[8 + c // 2, 2 * hh + c % 2] = out[:, hh]

        @pl.when(c % 2 == 1)
        def _():
            y_begin(c, 8 + c // 2)

    def chunk(c):
        @pl.when(b < nv - 1)
        def _():
            chunk_n(c)

            @pl.when(odd == 1)
            def _():
                pack_n(c, 4 + c, acc_n[...])

            @pl.when((odd == 0) & (c % 2 == 1))
            def _():
                pack_n(c, 4 + c // 2, acc_m[...] + acc_n[...])

            @pl.when((odd == 0) & (c % 2 == 0))
            def _():
                acc_m[...] = acc_n[...]

        @pl.when((odd == 0) & (b > 0))
        def _():
            chunk_p(c)

        @pl.when(odd == 1)
        def _():
            chunk_q(c)

    def n_copy(c):
        return pltpu.make_async_remote_copy(
            src_ref=fin.at[4 + c],
            dst_ref=fin_n.at[c % 2, y],
            send_sem=fn_s.at[c],
            recv_sem=fn_r.at[c % 2],
            device_id=at(2 + c // 2, z),
            device_id_type=MESH,
        )

    def o_copy():
        return pltpu.make_async_remote_copy(
            src_ref=fin.at[pl.ds(0, QUARTERS)],
            dst_ref=fin_o.at[y % 2],
            send_sem=fo_s.at[0],
            recv_sem=fo_r.at[y % 2],
            device_id=at(y // 2, z),
            device_id_type=MESH,
        )

    def p_copy():
        return pltpu.make_async_remote_copy(
            src_ref=fin.at[pl.ds(8, QUARTERS)],
            dst_ref=fin_p.at[y % 2],
            send_sem=fp_s.at[0],
            recv_sem=fp_r.at[y % 2],
            device_id={"samples": (2 + y // 2) * nz + z, "variants": jnp.maximum(b - 1, 0)},
            device_id_type=MESH,
        )

    def q_copy(k):
        return pltpu.make_async_remote_copy(
            src_ref=fin.at[8 + k],
            dst_ref=fin_p.at[y // 2, 2 * k + y % 2],
            send_sem=fp_s.at[k],
            recv_sem=fp_r.at[y // 2],
            device_id={"samples": 3 * nz + z, "variants": jnp.maximum(b - 1, 0)},
            device_id_type=MESH,
        )

    def n_final(c):
        owner = 2 + c // 2

        @pl.when(y == owner)
        def _():
            fin_n[c % 2, y] = fin[4 + c]

        @pl.when(y != owner)
        def _():
            n_copy(c).start()

    def step(c, carry):
        @pl.when(c < QUARTERS)
        def _():
            chunk(c)

        def both(i, action):
            @pl.when((odd == 1) & (b < nv - 1))
            def _():
                action(QUARTERS + i)

            @pl.when((odd == 0) & (b > 0))
            def _():
                action(2 * QUARTERS + i)

            @pl.when(i % 2 == 1)
            def _():
                action((1 + odd) * QUARTERS + i // 2)

        def own_units(action):
            for u in range(QUARTERS):
                action(u)

        @pl.when(c == 0)
        def _():
            own_units(y_relay)

        @pl.when(c == 1)
        def _():
            per_sample()
            both(0, y_relay)

        @pl.when(c == 2)
        def _():
            own_units(y_fold)
            both(1, y_relay)

        @pl.when(c == 3)
        def _():
            both(0, y_fold)
            both(1, y_fold)

        @pl.when(c == 4)
        def _():
            both(2, y_fold_all)
            both(3, y_fold_all)
            own_units(z_fold)

            @pl.when(y == 0)
            def _():
                fin_o[0] = fin[0:QUARTERS]

            @pl.when(y > 0)
            def _():
                o_copy().start()

        @pl.when(c == 4)
        def _():
            drain(samp_r.at[pl.ds(0, nv - 1)], samp_rs.at[0])
            samp_g[b] = sum(samp_r[p] for p in range(nv))
            for d in range(1, nv):
                samp_copy(1, samp_g.at[b], samp_g.at[b], (b + d) % nv).start()

        @pl.when(c > QUARTERS)
        def _():
            i = c - QUARTERS - 1
            both(i, z_fold)

            @pl.when((odd == 1) & (b < nv - 1))
            def _():
                n_final(i)

            @pl.when((odd == 0) & (i % 2 == 1))
            def _():
                n_final(i // 2)

        return carry

    lax.fori_loop(0, 2 * QUARTERS + 1, step, 0)

    @pl.when((odd == 0) & (b > 0))
    def _():
        p_copy().start()

    @pl.when(odd == 1)
    def _():
        for k_unit in range(2):
            q_copy(k_unit).start()

    drain(cnt_y.at[pl.ds(0, ny - 1)], stat_r.at[3])
    stat_o[4:8, :] = sum(cnt_y[i] for i in range(ny))
    drain(samp_g.at[pl.ds(0, nv - 1)], samp_rs.at[1])
    samp_o[...] = samp_g[...]

    @pl.when(y == 0)
    def _():
        drain(fin_o.at[1], fo_r.at[1])

    @pl.when(y == 1)
    def _():
        drain(fin_o.at[0], fo_r.at[0])
        drain(fin_o.at[1], fo_r.at[1])

    @pl.when(y < 2)
    def _():
        for h in range(2):
            for q in range(QUARTERS):
                ld_o[h * TILE : (h + 1) * TILE, q * qw : (q + 1) * qw] = fin_o[h, q]

    def wait_n():
        for h in range(2):
            drain(fin_n.at[h, pl.ds(0, ny - 1)], fn_r.at[h])

    def wait_p():
        for h in range(2):
            drain(fin_p.at[h], fp_r.at[h])

    def write(value):
        for h in range(2):
            for q in range(QUARTERS):
                ld_o[h * TILE : (h + 1) * TILE, q * qw : (q + 1) * qw] = value(h, q)

    @pl.when((y >= 2) & (odd == 1) & (b < nv - 1))
    def _():
        wait_n()
        wait_p()
        write(lambda h, q: fin_n[h, q] + fin_p[h, q])

    @pl.when((y == 2) & (odd == 0))
    def _():
        wait_n()
        write(lambda h, q: fin_n[h, q])

    @pl.when((y == 3) & (odd == 0))
    def _():
        wait_p()
        write(lambda h, q: fin_p[h, q])

    @pl.when((y >= 2) & (b == nv - 1))
    def _():
        ld_o[...] = jnp.zeros_like(ld_o)

    drain(crit_z.at[pl.ds(0, nz - 1)], stat_s.at[0])
    drain(cnt_z.at[pl.ds(0, nz - 1)], stat_s.at[1])
    drain(crit_y.at[pl.ds(0, ny - 1)], stat_s.at[2])
    drain(cnt_y.at[pl.ds(0, ny - 1)], stat_s.at[3])
    drain(samp_r.at[pl.ds(0, nv - 1)], samp_ss.at[0])
    drain(samp_g.at[pl.ds(0, nv - 1)], samp_ss.at[1])

    def sent(u, carry):
        drain(yfar.at[u], ya_s.at[u])
        drain(ynear.at[u], yb_s.at[u])
        drain(zrecv.at[u], zs_sem.at[u])
        return carry

    lax.fori_loop(0, QUARTERS, sent, 0)

    @pl.when(y > 0)
    def _():
        o_copy().wait_send()

    def sent_n(count):
        lax.fori_loop(QUARTERS, QUARTERS + count, sent, 0)
        for c in range(count):

            @pl.when(y != 2 + c // 2)
            def _():
                n_copy(c).wait_send()

    @pl.when((odd == 1) & (b < nv - 1))
    def _():
        sent_n(QUARTERS)

    @pl.when(odd == 0)
    def _():
        sent_n(2)
        for c in range(QUARTERS):
            copy_q(c).wait_send()

    @pl.when(b < nv - 1)
    def _():
        to_next.wait_send()
        for c in range(QUARTERS):
            copy_p(c).wait_send()

    @pl.when(b > 0)
    def _():
        to_prev.wait_send()
        for c in range(QUARTERS):
            copy_n(c).wait_send()

    @pl.when((odd == 0) & (b > 0))
    def _():
        lax.fori_loop(2 * QUARTERS, 3 * QUARTERS, sent, 0)
        p_copy().wait_send()

    @pl.when(odd == 1)
    def _():
        lax.fori_loop(2 * QUARTERS, 2 * QUARTERS + 2, sent, 0)
        for k_unit in range(2):
            q_copy(k_unit).wait_send()


def deliver(ratio, stat_ref, ld_ref, samp_ref, mean_o, var_o, count_o, ld_o, calls_o, share_o):
    mean_o[...] = stat_ref[0:1, :]
    var_o[...] = stat_ref[1:2, :]
    count_o[...] = stat_ref[4:8, :].astype(jnp.int32)
    ld_o[...] = ld_ref[...]
    slice_w = samp_ref.shape[2]
    for p in range(samp_ref.shape[0]):
        cols = slice(p * slice_w, (p + 1) * slice_w)
        calls_o[:, cols] = samp_ref[p, 0:2, :].astype(jnp.int32)
        share_o[:, cols] = samp_ref[p, 2:3, :] * ratio


def on_device(ny, nz, nv, genotypes, weights):
    rows, cols = genotypes.shape
    blocks = rows // TILE
    width, qw, slice_w = cols // PARTS, rows // QUARTERS, cols // nv
    half = PARTS // 2
    bf16 = jnp.bfloat16
    vmem = pl.BlockSpec(memory_space=pltpu.VMEM)
    dma = pltpu.SemaphoreType.DMA
    units = 3 * QUARTERS
    shapes = (((8, rows), F32), ((2 * TILE, rows), F32), ((nv, 4, slice_w), F32))
    held = pl.pallas_call(
        functools.partial(kernel, ny, nz, nv),
        out_shape=[jax.ShapeDtypeStruct(s, t) for s, t in shapes],
        in_specs=[pl.BlockSpec(memory_space=pl.ANY), vmem],
        out_specs=[vmem] * len(shapes),
        scratch_shapes=[
            pltpu.VMEM((blocks, TILE, cols), jnp.int32),
            pltpu.VMEM((PARTS, 2, nz, 2, TILE, width), bf16),
            pltpu.VMEM((rows, cols), bf16),
            pltpu.VMEM((cols, rows), bf16),
            pltpu.VMEM((nz * TILE, half * width), bf16),
            pltpu.VMEM((qw, cols), bf16),
            pltpu.VMEM((nz * TILE, rows), F32),
            pltpu.VMEM((nz * TILE, rows), F32),
            pltpu.VMEM((QUARTERS, half, nz // 2, 2, TILE, width), bf16),
            pltpu.VMEM((QUARTERS, half, nz, TILE, width), bf16),
            pltpu.VMEM((QUARTERS, half, nz // 2, 2, TILE, width), bf16),
            pltpu.VMEM((TILE, cols), F32),
            pltpu.VMEM((TILE, cols), F32),
            pltpu.VMEM((3, blocks, TILE, LANES), F32),
            pltpu.VMEM((blocks, TILE, LANES), jnp.int32),
            pltpu.VMEM((8, cols), jnp.int32),
            pltpu.VMEM((8, cols), F32),
            pltpu.VMEM((nz, 4, rows), F32),
            pltpu.VMEM((ny, 4, rows), F32),
            pltpu.VMEM((nz, 4, rows), F32),
            pltpu.VMEM((ny, 4, rows), F32),
            pltpu.VMEM((3, 2, rows), F32),
            pltpu.VMEM((3, 2, 2, nz, 2, TILE, LANES), F32),
            pltpu.VMEM((nv, 4, slice_w), F32),
            pltpu.VMEM((nv, 4, slice_w), F32),
            pltpu.VMEM((nv, 4, slice_w), F32),
            pltpu.VMEM((rows, rows // 2), F32),
            pltpu.VMEM((units, ny, nz, TILE, qw), HALF),
            pltpu.VMEM((units, 2, nz // 2, TILE, qw), HALF),
            pltpu.VMEM((units, 2, nz, TILE, qw), HALF),
            pltpu.VMEM((units, nz, TILE, qw), HALF),
            pltpu.VMEM((units, nz - 1, TILE, qw), HALF),
            pltpu.VMEM((units, TILE, qw), F32),
            pltpu.VMEM((2, QUARTERS, TILE, qw), F32),
            pltpu.VMEM((2, QUARTERS, TILE, qw), F32),
            pltpu.VMEM((2, QUARTERS, TILE, qw), F32),
            dma((8,)),
            dma((QUARTERS,)),
            dma((QUARTERS,)),
            dma((QUARTERS,)),
            dma((QUARTERS,)),
            dma((QUARTERS,)),
            dma((QUARTERS,)),
            dma((4,)),
            dma((4,)),
            dma((2,)),
            dma((2,)),
            dma((2,)),
            dma((2,)),
            dma((units,)),
            dma((units,)),
            dma((units,)),
            dma((units,)),
            dma((units,)),
            dma((units,)),
            dma((1,)),
            dma((2,)),
            dma((QUARTERS,)),
            dma((2,)),
            dma((2,)),
            dma((2,)),
        ],
        compiler_params=pltpu.CompilerParams(
            collective_id=0, has_side_effects=True, vmem_limit_bytes=60 * 2**20
        ),
    )(genotypes.reshape(blocks, TILE, cols), weights.reshape(1, cols))
    shapes = (
        ((1, rows), F32),
        ((1, rows), F32),
        ((4, rows), jnp.int32),
        ((2 * TILE, rows), F32),
        ((2, cols), jnp.int32),
        ((1, cols), F32),
    )
    mean, var, counts, ld, calls, share = pl.pallas_call(
        functools.partial(deliver, ny * nz * cols / (nv * rows)),
        out_shape=[jax.ShapeDtypeStruct(s, t) for s, t in shapes],
        in_specs=[vmem] * 3,
        out_specs=[vmem] * len(shapes),
    )(*held)
    return (
        mean.reshape(rows),
        var.reshape(rows),
        counts,
        ld,
        calls,
        share.reshape(cols),
    )


def solution(mesh):
    ny = 4
    return jax.shard_map(
        functools.partial(on_device, ny, mesh.shape["samples"] // ny, mesh.shape["variants"]),
        mesh=mesh,
        in_specs=(P("variants", "samples"), P("samples")),
        out_specs=(
            P("variants"),
            P("variants"),
            P(None, "variants"),
            P("samples", "variants"),
            P(None, "samples"),
            P("samples"),
        ),
        check_vma=False,
    )
```

```python
import functools

import jax
import jax.numpy as jnp
from jax import lax
from jax.experimental import pallas as pl
from jax.experimental.pallas import tpu as pltpu
from jax.sharding import PartitionSpec as P

MESH = pl.DeviceIdType.MESH
LANES = 128
PARTS = 8
QUARTERS = 4
TILE = 16
HALF = jnp.int16
STEPS = 32000.0
F32 = jnp.float32
NT = (((1,), (1,)), ((), ()))
NN = (((1,), (0,)), ((), ()))


def drain(ref, sem):
    pltpu.make_async_copy(ref, ref, sem).wait()


def far_first(size):
    return sorted(range(1, size), key=lambda d: -min(d, size - d))


def folded(value):
    return sum(value[:, i : i + LANES] for i in range(0, value.shape[1], LANES))


def coded(value):
    size = jnp.minimum(jnp.sqrt(jnp.abs(value)) * STEPS + 0.5, 32767.0).astype(jnp.int32)
    return jnp.where(value < 0.0, -size, size).astype(HALF)


def decoded(code):
    value = code.astype(jnp.int32).astype(F32)
    return value * jnp.abs(value)


def spread(value, width):
    return jnp.concatenate([value] * (width // LANES), axis=1)


def kernel(
    ny, nz, nv,
    g_hbm, w_ref,
    stat_o, ld_o, samp_o,
    gbuf, raw, scl, scl_t, scl_n, scl_p, acc_n, acc_m, recv_q, recv_n, recv_p, wide_w, root_w, moments, codes, col, squares,
    crit_z, crit_y, cnt_z, cnt_y, mf, bcast, samp_s, samp_r, samp_g, acc,
    ysend, yfar, ynear, zsend, zrecv, fin, fin_o, fin_n, fin_p,
    gsem, xs_q, xr_q, xs_n, xs_p, xr_n, xr_p, stat_s, stat_r, mf_s, mf_r, samp_ss, samp_rs,
    ya_s, ya_r, yb_s, yb_r, zs_sem, zr_sem, fo_s, fo_r, fn_s, fn_r, fp_s, fp_r,
):
    k, b = lax.axis_index("samples"), lax.axis_index("variants")
    y, z = k // nz, k % nz
    blocks = 4 * nz
    rows = blocks * TILE
    width = gbuf.shape[2] // PARTS
    half = PARTS // 2
    slice_w = gbuf.shape[2] // nv
    first, last = b == 0, b == nv - 1

    def at(ky, kz):
        return {"samples": ky * nz + kz}

    for part in range(8):
        group = pl.ds(part * (blocks // 8), blocks // 8)
        pltpu.make_async_copy(g_hbm.at[group], gbuf.at[group], gsem.at[part]).start()

    barrier = pltpu.get_barrier_semaphore()

    def greet(device):
        pl.semaphore_signal(barrier, inc=1, device_id=device, device_id_type=MESH)

    for d in far_first(nz):
        greet(at(y, (z + d) % nz))
    for d in far_first(ny):
        greet(at((y + d) % ny, z))
    for d in range(1, nv):
        greet({"variants": (b + d) % nv})

    @pl.when(b > 0)
    def _():
        for d in far_first(ny):
            greet({"samples": ((y + d) % ny) * nz + z, "variants": b - 1})

    @pl.when(b < nv - 1)
    def _():
        for d in far_first(ny):
            greet({"samples": ((y + d) % ny) * nz + z, "variants": b + 1})

    wide_w[...] = jnp.broadcast_to(w_ref[...], wide_w.shape)
    root_w[...] = jnp.sqrt(wide_w[...])
    col[...] = jnp.zeros_like(col)
    squares[...] = jnp.zeros_like(squares)

    def place(rb):
        return rb // (2 * nz), (rb // 2) % nz, rb % 2

    def first_pass(rb, carry):
        yr, zz, hh = place(rb)
        sum_w = jnp.zeros((TILE, LANES), F32)
        sum_1 = jnp.zeros((TILE, LANES), F32)
        sum_2 = jnp.zeros((TILE, LANES), F32)
        for kc in range(PARTS):
            cols = slice(kc * width, (kc + 1) * width)
            g = gbuf[rb, :, cols]
            gf = g.astype(F32)
            raw[kc, yr, zz, hh] = gf.astype(jnp.bfloat16)
            kept = jnp.where(g == 3, 0.0, wide_w[:, cols])
            once = kept * gf
            twice = once * gf
            sum_w += folded(kept)
            sum_1 += folded(once)
            sum_2 += folded(twice)
        moments[0, rb] = sum_w
        moments[1, rb] = sum_1
        moments[2, rb] = sum_2
        return carry

    def count_pass(rb, carry):
        sum_c = jnp.zeros((TILE, LANES), jnp.int32)
        for kc in range(PARTS):
            cols = slice(kc * width, (kc + 1) * width)
            g = gbuf[rb, :, cols]
            code = jnp.left_shift(jnp.ones_like(g), g * 8)
            col[:, cols] += code[:8] + code[8:]
            sum_c += folded(code)
        codes[rb] = sum_c
        return carry

    odd = b % 2

    def copy_n(c):
        return pltpu.make_async_remote_copy(
            src_ref=raw.at[
                pl.ds(odd * (c % 2) * half, half),
                (1 - odd) * (c // 2),
                :,
                odd * (c // 2) + (1 - odd) * (c % 2),
            ],
            dst_ref=recv_n.at[c],
            send_sem=xs_n.at[c],
            recv_sem=xr_n.at[c],
            device_id={"variants": jnp.maximum(b - 1, 0)},
            device_id_type=MESH,
        )

    def copy_rows(c, base, dst, send_sems, recv_sems):
        return pltpu.make_async_remote_copy(
            src_ref=raw.at[pl.ds(base, half), c // 2, pl.ds((c % 2) * (nz // 2), nz // 2)],
            dst_ref=dst.at[c],
            send_sem=send_sems.at[c],
            recv_sem=recv_sems.at[c],
            device_id={"variants": jnp.minimum(b + 1, nv - 1)},
            device_id_type=MESH,
        )

    def copy_p(c):
        return copy_rows(c, half, recv_p, xs_p, xr_p)

    def copy_q(c):
        return copy_rows(c, 0, recv_q, xs_q, xr_q)

    def wait_part(part):
        group = pl.ds(part * (blocks // 8), blocks // 8)
        pltpu.make_async_copy(g_hbm.at[group], gbuf.at[group], gsem.at[part]).wait()

    neighbours = jnp.where(b > 0, ny - 1, 0) + jnp.where(b < nv - 1, ny - 1, 0)
    for part in range(8):
        wait_part(part)
        lax.fori_loop(part * (blocks // 8), (part + 1) * (blocks // 8), first_pass, 0)

    def start_chunk(c):
        @pl.when(b < nv - 1)
        def _():
            copy_p(c).start()

        @pl.when(odd == 0)
        def _():
            copy_q(c).start()

        @pl.when(b > 0)
        def _():
            copy_n(c).start()

    def to_row(value):
        return jnp.sum(value.reshape(rows, LANES).T, axis=0, keepdims=True)

    def push(src, dst, i, device):
        return pltpu.make_async_remote_copy(
            src_ref=src,
            dst_ref=dst,
            send_sem=stat_s.at[i],
            recv_sem=stat_r.at[i],
            device_id=device,
            device_id_type=MESH,
        )

    for q in range(3):
        crit_z[z, q : q + 1, :] = to_row(moments[q])
    crit_z[z, 3:4, :] = jnp.zeros((1, rows), F32)
    pl.semaphore_wait(barrier, (ny - 1) + (nz - 1) + (nv - 1) + neighbours)
    for d in far_first(nz):
        push(crit_z.at[z], crit_z.at[z], 0, at(y, (z + d) % nz)).start()
    start_chunk(0)
    start_chunk(1)
    lax.fori_loop(0, blocks, count_pass, 0)
    fields = codes[...]
    for level in range(4):
        field = jnp.bitwise_and(jnp.right_shift(fields, 8 * level), 255)
        cnt_z[z, level : level + 1, :] = to_row(field.astype(F32))
    for d in far_first(nz):
        push(cnt_z.at[z], cnt_z.at[z], 1, at(y, (z + d) % nz)).start()

    drain(crit_z.at[pl.ds(0, nz - 1)], stat_r.at[0])
    crit_y[y] = sum(crit_z[i] for i in range(nz))
    for d in far_first(ny):
        push(crit_y.at[y], crit_y.at[y], 2, at((y + d) % ny, z)).start()
    drain(crit_y.at[pl.ds(0, ny - 1)], stat_r.at[2])
    total = sum(crit_y[i] for i in range(ny))
    w_sum, first_total, second_total = total[0:1], total[1:2], total[2:3]
    mean = first_total / w_sum
    var = (second_total - first_total * mean) / w_sum
    factor = 1.0 / jnp.sqrt(w_sum * (var + 1e-05))
    stat_o[0:1, :] = mean
    stat_o[1:2, :] = var
    stat_o[2:4, :] = jnp.zeros((2, rows), F32)
    mf[0, 0:1, :] = mean
    mf[0, 1:2, :] = factor

    def mf_copy(slot, target):
        return pltpu.make_async_remote_copy(
            src_ref=mf.at[0],
            dst_ref=mf.at[slot],
            send_sem=mf_s.at[slot - 1],
            recv_sem=mf_r.at[slot - 1],
            device_id={"variants": target},
            device_id_type=MESH,
        )

    to_prev = mf_copy(1, jnp.maximum(b - 1, 0))
    to_next = mf_copy(2, jnp.minimum(b + 1, nv - 1))

    @pl.when(b > 0)
    def _():
        to_prev.start()

    @pl.when(b < nv - 1)
    def _():
        to_next.start()

    start_chunk(2)
    start_chunk(3)

    def widen(slot):
        for q in range(2):
            tall = jnp.broadcast_to(mf[slot, q : q + 1, :], (LANES, rows)).T
            bcast[slot, q] = tall.reshape(2, nz, 2, TILE, LANES)

    def scaled(value, roots, mean_rows, factor_rows):
        x = value.astype(F32)
        out = (roots * (x - spread(mean_rows, width))) * spread(factor_rows, width)
        return jnp.where(x > 2.5, 0.0, out).astype(jnp.bfloat16)

    widen(0)

    drain(cnt_z.at[pl.ds(0, nz - 1)], stat_r.at[1])
    cnt_y[y] = sum(cnt_z[i] for i in range(nz))
    for d in far_first(ny):
        push(cnt_y.at[y], cnt_y.at[y], 3, at((y + d) % ny, z)).start()

    def second_pass(rb, carry):
        yr, zz, hh = place(rb)
        mean_rows, factor_rows = bcast[0, 0, yr, zz, hh], bcast[0, 1, yr, zz, hh]
        for kc in range(PARTS):
            cols = slice(kc * width, (kc + 1) * width)
            out = scaled(raw[kc, yr, zz, hh], root_w[:, cols], mean_rows, factor_rows)
            scl[pl.ds(pl.multiple_of(rb * TILE, TILE), TILE), cols] = out
        return carry

    def square_pass(rb, carry):
        for kc in range(PARTS):
            cols = slice(kc * width, (kc + 1) * width)
            wide = scl[pl.ds(pl.multiple_of(rb * TILE, TILE), TILE), cols].astype(F32)
            wide = wide * wide
            squares[:, cols] += wide[:8] + wide[8:]
        return carry

    lax.fori_loop(0, blocks, second_pass, 0)

    def samp_copy(i, src, dst, target):
        return pltpu.make_async_remote_copy(
            src_ref=src,
            dst_ref=dst,
            send_sem=samp_ss.at[i],
            recv_sem=samp_rs.at[i],
            device_id={"variants": target},
            device_id_type=MESH,
        )

    def per_sample():
        lax.fori_loop(0, blocks, square_pass, 0)
        packed = col[...]
        missing = jnp.sum(jnp.bitwise_and(jnp.right_shift(packed, 24), 255), axis=0, keepdims=True)
        het = jnp.sum(jnp.bitwise_and(jnp.right_shift(packed, 8), 255), axis=0, keepdims=True)
        called = (rows - missing).astype(F32)
        het = het.astype(F32)
        share = jnp.sum(squares[...], axis=0, keepdims=True)
        for p in range(nv):
            cols = slice(p * slice_w, (p + 1) * slice_w)
            samp_s[p, 0:1, :] = called[:, cols]
            samp_s[p, 1:2, :] = het[:, cols]
            samp_s[p, 2:3, :] = share[:, cols]
            samp_s[p, 3:4, :] = jnp.zeros((1, slice_w), F32)
        samp_r[b] = samp_s[b]
        for d in range(1, nv):
            target = (b + d) % nv
            samp_copy(0, samp_s.at[target], samp_r.at[b], target).start()

    up, down, across = (y + 1) % ny, (y + ny - 1) % ny, (y + 2) % ny
    lower, upper = pl.ds(0, nz // 2), pl.ds(nz // 2, nz // 2)

    def y_copy(src, dst, sems, target):
        return pltpu.make_async_remote_copy(
            src_ref=src,
            dst_ref=dst,
            send_sem=sems[0],
            recv_sem=sems[1],
            device_id=at(target, z),
            device_id_type=MESH,
        )

    def z_copy(u, d):
        target = (z + d) % nz
        return pltpu.make_async_remote_copy(
            src_ref=zsend.at[u, target],
            dst_ref=zrecv.at[u, d - 1],
            send_sem=zs_sem.at[u],
            recv_sem=zr_sem.at[u],
            device_id=at(y, target),
            device_id_type=MESH,
        )

    def y_start(u):
        sems = ya_s.at[u], ya_r.at[u]
        y_copy(ysend.at[u, across, lower], yfar.at[u, 0], sems, up).start()
        y_copy(ysend.at[u, across, upper], yfar.at[u, 1], sems, down).start()

    def y_direct(u):
        far, near = (ya_s.at[u], ya_r.at[u]), (yb_s.at[u], yb_r.at[u])
        y_copy(ysend.at[u, across, lower], yfar.at[u, 0], far, across).start()
        y_copy(ysend.at[u, across, upper], yfar.at[u, 1], far, across).start()
        y_copy(ysend.at[u, up], ynear.at[u, 0], near, up).start()
        y_copy(ysend.at[u, down], ynear.at[u, 1], near, down).start()

    def y_relay(u):
        drain(yfar.at[u], ya_r.at[u])
        sems = yb_s.at[u], yb_r.at[u]
        for slot, target, part in ((0, up, lower), (1, down, upper)):
            both = decoded(ysend[u, target, part]) + decoded(yfar[u, slot])
            ysend[u, target, part] = coded(both * (1.0 / STEPS**2))
            y_copy(ysend.at[u, target], ynear.at[u, slot], sems, target).start()

    def z_start(u, part):
        zsend[u] = coded(part * (1.0 / STEPS**2))
        for d in far_first(nz):
            z_copy(u, d).start()

    def y_fold_all(u):
        drain(ynear.at[u], yb_r.at[u])
        drain(yfar.at[u], ya_r.at[u])
        part = decoded(ysend[u, y]) + decoded(ynear[u, 0]) + decoded(ynear[u, 1])
        z_start(u, part + decoded(yfar[u]).reshape(nz, TILE, qw))

    def y_fold(u):
        drain(ynear.at[u], yb_r.at[u])
        z_start(u, decoded(ysend[u, y]) + decoded(ynear[u, 0]) + decoded(ynear[u, 1]))

    def z_fold(u):
        drain(zrecv.at[u], zr_sem.at[u])
        part = decoded(zsend[u, z])
        for d in range(nz - 1):
            part = part + decoded(zrecv[u, d])
        fin[u] = part * (1.0 / STEPS**2)

    qw = rows // QUARTERS

    def group_rows(value, u):
        value = coded(value).reshape(2, nz, 2, TILE, qw)
        for yr in range(2):
            for hh in range(2):
                ysend[u, 2 * yr + hh] = value[yr, :, hh]

    for pair in range(2):
        with jax.named_scope("own_dot"):
            if pair == 0:
                acc[...] = lax.dot_general(
                    scl[...], scl[: rows // 2], NT, preferred_element_type=F32
                )
            else:
                acc[: rows // 2] = acc[rows // 2 :].T
                acc[rows // 2 :] = lax.dot_general(
                    scl[rows // 2 :], scl[rows // 2 :], NT, preferred_element_type=F32
                )
        for j in range(2):
            group_rows(acc[:, j * qw : (j + 1) * qw], 2 * pair + j)
            y_start(2 * pair + j)

    @pl.when(b < nv - 1)
    def _():
        with jax.named_scope("turn"):
            scl_t[: half * width] = scl[:, : half * width].T

            @pl.when(odd == 0)
            def _():
                scl_t[half * width :] = scl[:, half * width :].T

        to_prev.wait_recv()
        widen(1)

    @pl.when(b > 0)
    def _():
        to_next.wait_recv()
        widen(2)

    def y_begin(c, u):
        @pl.when(c < QUARTERS - 2)
        def _():
            y_start(u)

        @pl.when(c >= QUARTERS - 2)
        def _():
            y_direct(u)

    def chunk_n(c):
        copy_n(c).wait_recv()
        side = (1 - odd) * (c % 2)
        yr, hh = odd * (c // 2), odd * (c % 2) + (1 - odd) * (c // 2)
        base = pl.multiple_of(side * half * width, half * width)
        for kc in range(half):
            roots = root_w[:, pl.ds(pl.multiple_of(base + kc * width, width), width)]
            for zz in range(nz):
                scl_n[zz * TILE : (zz + 1) * TILE, kc * width : (kc + 1) * width] = scaled(
                    recv_n[c, kc, zz], roots, bcast[1, 0, yr, zz, hh], bcast[1, 1, yr, zz, hh]
                )
        acc_n[...] = lax.dot_general(
            scl_n[...], scl_t[pl.ds(base, half * width)], NN, preferred_element_type=F32
        )

    def pack_n(c, u, out):
        out = coded(out)
        for q in range(QUARTERS):
            ysend[u, q] = out[:, q * qw : (q + 1) * qw].reshape(nz, TILE, qw)
        y_begin(c, u)

    def turn_p(c, buf, base):
        for kc in range(half):
            cols = slice((base + kc) * width, (base + kc + 1) * width)
            roots = root_w[:, cols]
            for zz in range(nz // 2):
                for hh in range(2):
                    spot = (c // 2, (c % 2) * (nz // 2) + zz, hh)
                    start = (2 * zz + hh) * TILE
                    scl_p[start : start + TILE, cols] = scaled(
                        buf[c, kc, zz, hh], roots, bcast[(2, 0, *spot)], bcast[(2, 1, *spot)]
                    )

    def chunk_p(c):
        copy_p(c).wait_recv()
        turn_p(c, recv_p, half)
        out = lax.dot_general(
            scl[:, half * width :], scl_p[:, half * width :], NT, preferred_element_type=F32
        )
        group_rows(out, 8 + c)
        y_begin(c, 8 + c)

    def chunk_q(c):
        copy_p(c).wait_recv()
        turn_p(c, recv_p, half)
        copy_q(c).wait_recv()
        turn_p(c, recv_q, 0)
        out = lax.dot_general(
            scl[rows // 2 :], scl_p[...], NT, preferred_element_type=F32
        )
        out = coded(out).reshape(nz, 2, TILE, qw)
        for hh in range(2):
            ysend[8 + c // 2, 2 * hh + c % 2] = out[:, hh]

        @pl.when(c % 2 == 1)
        def _():
            y_begin(c, 8 + c // 2)

    def chunk(c):
        @pl.when(b < nv - 1)
        def _():
            chunk_n(c)

            @pl.when(odd == 1)
            def _():
                pack_n(c, 4 + c, acc_n[...])

            @pl.when((odd == 0) & (c % 2 == 1))
            def _():
                pack_n(c, 4 + c // 2, acc_m[...] + acc_n[...])

            @pl.when((odd == 0) & (c % 2 == 0))
            def _():
                acc_m[...] = acc_n[...]

        @pl.when((odd == 0) & (b > 0))
        def _():
            chunk_p(c)

        @pl.when(odd == 1)
        def _():
            chunk_q(c)

    def n_copy(c):
        return pltpu.make_async_remote_copy(
            src_ref=fin.at[4 + c],
            dst_ref=fin_n.at[c % 2, y],
            send_sem=fn_s.at[c],
            recv_sem=fn_r.at[c % 2],
            device_id=at(2 + c // 2, z),
            device_id_type=MESH,
        )

    def o_copy():
        return pltpu.make_async_remote_copy(
            src_ref=fin.at[pl.ds(0, QUARTERS)],
            dst_ref=fin_o.at[y % 2],
            send_sem=fo_s.at[0],
            recv_sem=fo_r.at[y % 2],
            device_id=at(y // 2, z),
            device_id_type=MESH,
        )

    def p_copy():
        return pltpu.make_async_remote_copy(
            src_ref=fin.at[pl.ds(8, QUARTERS)],
            dst_ref=fin_p.at[y % 2],
            send_sem=fp_s.at[0],
            recv_sem=fp_r.at[y % 2],
            device_id={"samples": (2 + y // 2) * nz + z, "variants": jnp.maximum(b - 1, 0)},
            device_id_type=MESH,
        )

    def q_copy(k):
        return pltpu.make_async_remote_copy(
            src_ref=fin.at[8 + k],
            dst_ref=fin_p.at[y // 2, 2 * k + y % 2],
            send_sem=fp_s.at[k],
            recv_sem=fp_r.at[y // 2],
            device_id={"samples": 3 * nz + z, "variants": jnp.maximum(b - 1, 0)},
            device_id_type=MESH,
        )

    def n_final(c):
        owner = 2 + c // 2

        @pl.when(y == owner)
        def _():
            fin_n[c % 2, y] = fin[4 + c]

        @pl.when(y != owner)
        def _():
            n_copy(c).start()

    def step(c, carry):
        @pl.when(c < QUARTERS)
        def _():
            chunk(c)

        def both(i, action):
            @pl.when((odd == 1) & (b < nv - 1))
            def _():
                action(QUARTERS + i)

            @pl.when((odd == 0) & (b > 0))
            def _():
                action(2 * QUARTERS + i)

            @pl.when(i % 2 == 1)
            def _():
                action((1 + odd) * QUARTERS + i // 2)

        def own_units(action):
            for u in range(QUARTERS):
                action(u)

        @pl.when(c == 0)
        def _():
            own_units(y_relay)

        @pl.when(c == 1)
        def _():
            per_sample()
            both(0, y_relay)

        @pl.when(c == 2)
        def _():
            own_units(y_fold)
            both(1, y_relay)

        @pl.when(c == 3)
        def _():
            both(0, y_fold)
            both(1, y_fold)

        @pl.when(c == 4)
        def _():
            both(2, y_fold_all)
            both(3, y_fold_all)
            own_units(z_fold)

            @pl.when(y == 0)
            def _():
                fin_o[0] = fin[0:QUARTERS]

            @pl.when(y > 0)
            def _():
                o_copy().start()

        @pl.when(c == 4)
        def _():
            drain(samp_r.at[pl.ds(0, nv - 1)], samp_rs.at[0])
            samp_g[b] = sum(samp_r[p] for p in range(nv))
            for d in range(1, nv):
                samp_copy(1, samp_g.at[b], samp_g.at[b], (b + d) % nv).start()

        @pl.when(c > QUARTERS)
        def _():
            i = c - QUARTERS - 1
            both(i, z_fold)

            @pl.when((odd == 1) & (b < nv - 1))
            def _():
                n_final(i)

            @pl.when((odd == 0) & (i % 2 == 1))
            def _():
                n_final(i // 2)

        return carry

    lax.fori_loop(0, 2 * QUARTERS + 1, step, 0)

    @pl.when((odd == 0) & (b > 0))
    def _():
        p_copy().start()

    @pl.when(odd == 1)
    def _():
        for k_unit in range(2):
            q_copy(k_unit).start()

    drain(cnt_y.at[pl.ds(0, ny - 1)], stat_r.at[3])
    stat_o[4:8, :] = sum(cnt_y[i] for i in range(ny))
    drain(samp_g.at[pl.ds(0, nv - 1)], samp_rs.at[1])
    samp_o[...] = samp_g[...]

    @pl.when(y == 0)
    def _():
        drain(fin_o.at[1], fo_r.at[1])

    @pl.when(y == 1)
    def _():
        drain(fin_o.at[0], fo_r.at[0])
        drain(fin_o.at[1], fo_r.at[1])

    @pl.when(y < 2)
    def _():
        for h in range(2):
            for q in range(QUARTERS):
                ld_o[h * TILE : (h + 1) * TILE, q * qw : (q + 1) * qw] = fin_o[h, q]

    def wait_n():
        for h in range(2):
            drain(fin_n.at[h, pl.ds(0, ny - 1)], fn_r.at[h])

    def wait_p():
        for h in range(2):
            drain(fin_p.at[h], fp_r.at[h])

    def write(value):
        for h in range(2):
            for q in range(QUARTERS):
                ld_o[h * TILE : (h + 1) * TILE, q * qw : (q + 1) * qw] = value(h, q)

    @pl.when((y >= 2) & (odd == 1) & (b < nv - 1))
    def _():
        wait_n()
        wait_p()
        write(lambda h, q: fin_n[h, q] + fin_p[h, q])

    @pl.when((y == 2) & (odd == 0))
    def _():
        wait_n()
        write(lambda h, q: fin_n[h, q])

    @pl.when((y == 3) & (odd == 0))
    def _():
        wait_p()
        write(lambda h, q: fin_p[h, q])

    @pl.when((y >= 2) & (b == nv - 1))
    def _():
        ld_o[...] = jnp.zeros_like(ld_o)

    drain(crit_z.at[pl.ds(0, nz - 1)], stat_s.at[0])
    drain(cnt_z.at[pl.ds(0, nz - 1)], stat_s.at[1])
    drain(crit_y.at[pl.ds(0, ny - 1)], stat_s.at[2])
    drain(cnt_y.at[pl.ds(0, ny - 1)], stat_s.at[3])
    drain(samp_r.at[pl.ds(0, nv - 1)], samp_ss.at[0])
    drain(samp_g.at[pl.ds(0, nv - 1)], samp_ss.at[1])

    def sent(u, carry):
        drain(yfar.at[u], ya_s.at[u])
        drain(ynear.at[u], yb_s.at[u])
        drain(zrecv.at[u], zs_sem.at[u])
        return carry

    lax.fori_loop(0, QUARTERS, sent, 0)

    @pl.when(y > 0)
    def _():
        o_copy().wait_send()

    def sent_n(count):
        lax.fori_loop(QUARTERS, QUARTERS + count, sent, 0)
        for c in range(count):

            @pl.when(y != 2 + c // 2)
            def _():
                n_copy(c).wait_send()

    @pl.when((odd == 1) & (b < nv - 1))
    def _():
        sent_n(QUARTERS)

    @pl.when(odd == 0)
    def _():
        sent_n(2)
        for c in range(QUARTERS):
            copy_q(c).wait_send()

    @pl.when(b < nv - 1)
    def _():
        to_next.wait_send()
        for c in range(QUARTERS):
            copy_p(c).wait_send()

    @pl.when(b > 0)
    def _():
        to_prev.wait_send()
        for c in range(QUARTERS):
            copy_n(c).wait_send()

    @pl.when((odd == 0) & (b > 0))
    def _():
        lax.fori_loop(2 * QUARTERS, 3 * QUARTERS, sent, 0)
        p_copy().wait_send()

    @pl.when(odd == 1)
    def _():
        lax.fori_loop(2 * QUARTERS, 2 * QUARTERS + 2, sent, 0)
        for k_unit in range(2):
            q_copy(k_unit).wait_send()


def deliver(ratio, stat_ref, ld_ref, samp_ref, mean_o, var_o, count_o, ld_o, calls_o, share_o):
    mean_o[...] = stat_ref[0:1, :]
    var_o[...] = stat_ref[1:2, :]
    count_o[...] = stat_ref[4:8, :].astype(jnp.int32)
    ld_o[...] = ld_ref[...]
    slice_w = samp_ref.shape[2]
    for p in range(samp_ref.shape[0]):
        cols = slice(p * slice_w, (p + 1) * slice_w)
        calls_o[:, cols] = samp_ref[p, 0:2, :].astype(jnp.int32)
        share_o[:, cols] = samp_ref[p, 2:3, :] * ratio


def on_device(ny, nz, nv, genotypes, weights):
    rows, cols = genotypes.shape
    blocks = rows // TILE
    width, qw, slice_w = cols // PARTS, rows // QUARTERS, cols // nv
    half = PARTS // 2
    bf16 = jnp.bfloat16
    vmem = pl.BlockSpec(memory_space=pltpu.VMEM)
    dma = pltpu.SemaphoreType.DMA
    units = 3 * QUARTERS
    shapes = (((8, rows), F32), ((2 * TILE, rows), F32), ((nv, 4, slice_w), F32))
    held = pl.pallas_call(
        functools.partial(kernel, ny, nz, nv),
        out_shape=[jax.ShapeDtypeStruct(s, t) for s, t in shapes],
        in_specs=[pl.BlockSpec(memory_space=pl.ANY), vmem],
        out_specs=[vmem] * len(shapes),
        scratch_shapes=[
            pltpu.VMEM((blocks, TILE, cols), jnp.int32),
            pltpu.VMEM((PARTS, 2, nz, 2, TILE, width), bf16),
            pltpu.VMEM((rows, cols), bf16),
            pltpu.VMEM((cols, rows), bf16),
            pltpu.VMEM((nz * TILE, half * width), bf16),
            pltpu.VMEM((qw, cols), bf16),
            pltpu.VMEM((nz * TILE, rows), F32),
            pltpu.VMEM((nz * TILE, rows), F32),
            pltpu.VMEM((QUARTERS, half, nz // 2, 2, TILE, width), bf16),
            pltpu.VMEM((QUARTERS, half, nz, TILE, width), bf16),
            pltpu.VMEM((QUARTERS, half, nz // 2, 2, TILE, width), bf16),
            pltpu.VMEM((TILE, cols), F32),
            pltpu.VMEM((TILE, cols), F32),
            pltpu.VMEM((3, blocks, TILE, LANES), F32),
            pltpu.VMEM((blocks, TILE, LANES), jnp.int32),
            pltpu.VMEM((8, cols), jnp.int32),
            pltpu.VMEM((8, cols), F32),
            pltpu.VMEM((nz, 4, rows), F32),
            pltpu.VMEM((ny, 4, rows), F32),
            pltpu.VMEM((nz, 4, rows), F32),
            pltpu.VMEM((ny, 4, rows), F32),
            pltpu.VMEM((3, 2, rows), F32),
            pltpu.VMEM((3, 2, 2, nz, 2, TILE, LANES), F32),
            pltpu.VMEM((nv, 4, slice_w), F32),
            pltpu.VMEM((nv, 4, slice_w), F32),
            pltpu.VMEM((nv, 4, slice_w), F32),
            pltpu.VMEM((rows, rows // 2), F32),
            pltpu.VMEM((units, ny, nz, TILE, qw), HALF),
            pltpu.VMEM((units, 2, nz // 2, TILE, qw), HALF),
            pltpu.VMEM((units, 2, nz, TILE, qw), HALF),
            pltpu.VMEM((units, nz, TILE, qw), HALF),
            pltpu.VMEM((units, nz - 1, TILE, qw), HALF),
            pltpu.VMEM((units, TILE, qw), F32),
            pltpu.VMEM((2, QUARTERS, TILE, qw), F32),
            pltpu.VMEM((2, QUARTERS, TILE, qw), F32),
            pltpu.VMEM((2, QUARTERS, TILE, qw), F32),
            dma((8,)),
            dma((QUARTERS,)),
            dma((QUARTERS,)),
            dma((QUARTERS,)),
            dma((QUARTERS,)),
            dma((QUARTERS,)),
            dma((QUARTERS,)),
            dma((4,)),
            dma((4,)),
            dma((2,)),
            dma((2,)),
            dma((2,)),
            dma((2,)),
            dma((units,)),
            dma((units,)),
            dma((units,)),
            dma((units,)),
            dma((units,)),
            dma((units,)),
            dma((1,)),
            dma((2,)),
            dma((QUARTERS,)),
            dma((2,)),
            dma((2,)),
            dma((2,)),
        ],
        compiler_params=pltpu.CompilerParams(
            collective_id=0, has_side_effects=True, vmem_limit_bytes=60 * 2**20
        ),
    )(genotypes.reshape(blocks, TILE, cols), weights.reshape(1, cols))
    shapes = (
        ((1, rows), F32),
        ((1, rows), F32),
        ((4, rows), jnp.int32),
        ((2 * TILE, rows), F32),
        ((2, cols), jnp.int32),
        ((1, cols), F32),
    )
    mean, var, counts, ld, calls, share = pl.pallas_call(
        functools.partial(deliver, ny * nz * cols / (nv * rows)),
        out_shape=[jax.ShapeDtypeStruct(s, t) for s, t in shapes],
        in_specs=[vmem] * 3,
        out_specs=[vmem] * len(shapes),
    )(*held)
    return (
        mean.reshape(rows),
        var.reshape(rows),
        counts,
        ld,
        calls,
        share.reshape(cols),
    )


def solution(mesh):
    ny = 4
    return jax.shard_map(
        functools.partial(on_device, ny, mesh.shape["samples"] // ny, mesh.shape["variants"]),
        mesh=mesh,
        in_specs=(P("variants", "samples"), P("samples")),
        out_specs=(
            P("variants"),
            P("variants"),
            P(None, "variants"),
            P("samples", "variants"),
            P(None, "samples"),
            P("samples"),
        ),
        check_vma=False,
    )
```
